32 devices in a mesh: section: 8 (over z, x), dp: 4 (over y, core).
Axes of the slice: x: 2, y: 2, z: 4, core: 2. Of those that a mesh axis runs over, the one named last changes fastest.
Arguments:
- carry_act: bfloat16 [8, 32, 2304], P('section', 'dp'), may hold values from -6 to 6
- carry_act_tan: bfloat16 [8, 32, 2304], P('section', 'dp'), may hold values from -6 to 6
- carry_adj: bfloat16 [8, 32, 2304], P('section', 'dp'), may hold values from -0.75 to 0.75
- carry_adj_tan: bfloat16 [8, 32, 2304], P('section', 'dp'), may hold values from -0.75 to 0.75
- fresh_act: bfloat16 [2, 32, 2304], P(None, 'dp'), may hold values from -6 to 6
- loss_cot: bfloat16 [2, 32, 2304], P(None, 'dp'), may hold values from -0.75 to 0.75
- stash_act: bfloat16 [8, 2, 32, 2304], P('section', None, 'dp'), may hold values from -6 to 6
- stash_act_tan: bfloat16 [8, 2, 32, 2304], P('section', None, 'dp'), may hold values from -6 to 6
- norm_gain: bfloat16 [8, 2304], P('section'), may hold values from 0.25 to 1.75
- up_weight: bfloat16 [8, 2304, 4608], P('section', None, 'dp'), may hold values from -0.125 to 0.125
- down_weight: bfloat16 [8, 4608, 2304], P('section', 'dp'), may hold values from -0.09375 to 0.09375
- up_dir: bfloat16 [8, 2304, 4608], P('section', None, 'dp'), may hold values from -0.125 to 0.125
- down_dir: bfloat16 [8, 4608, 2304], P('section', 'dp'), may hold values from -0.09375 to 0.09375
Outputs:
- next_act: bfloat16 [8, 32, 2304], P('section', 'dp')
- next_act_tan: bfloat16 [8, 32, 2304], P('section', 'dp')
- next_adj: bfloat16 [8, 32, 2304], P('section', 'dp')
- next_adj_tan: bfloat16 [8, 32, 2304], P('section', 'dp')
- hvp_up: bfloat16 [8, 2304, 4608], P('section', None, 'dp')
- hvp_down: bfloat16 [8, 4608, 2304], P('section', 'dp')
The draws below stay inside these ranges and needn't reach their ends.
All inputs are finite; a program needn't handle non-finite values.
Results may differ from the reference program's by a relative error of at most 0.02.
Values may be sent and summed in bfloat16 or wider, within the bound.
No kernel may reach another device: no remote copies, remote signals or barrier semaphores. Data moves between devices by JAX's collectives and lax.ppermute only.
A program may use at most 128 MiB of HBM per device.

```python
import jax
import jax.numpy as jnp
from jax import lax

D = 2304
FF = 4608
TICKS = 2
TOKENS = 32
SECTIONS = 8
N_DP = 4


def block_levels(key, dims, split, low, top_value):
    factor_of = 1.0
    for position, blocks in split:
        draws = jax.random.uniform(jax.random.fold_in(jax.random.fold_in(key, 6), position), (blocks,), jnp.float32, low / len(split), top_value / len(split))
        factor_of = factor_of * jnp.repeat(jnp.exp(draws), dims[position] // blocks).reshape((-1,) + (1,) * (len(dims) - 1 - position))
    return factor_of


def noise(own_key, dims, scale, reach, cuts=(), dtype=jnp.bfloat16):
    entries = scale * jax.random.normal(own_key, dims, jnp.float32)
    if cuts:
        entries = entries * block_levels(own_key, dims, cuts, -0.22, 0.18)
    return jnp.clip(entries, -reach, reach).astype(dtype)


def setup_inputs(seed: int = 0) -> dict:
    splits = jax.random.split(jax.random.key(seed), 14)
    carry_act = noise(splits[0], (SECTIONS, TOKENS, D), 1.0, 6.0, ((0, 8), (1, 4)))
    carry_act_tan = noise(splits[1], (SECTIONS, TOKENS, D), 1.0, 6.0, ((0, 8), (1, 4)))
    carry_adj = noise(splits[2], (SECTIONS, TOKENS, D), 0.125, 0.75, ((0, 8), (1, 4)))
    carry_adj_tan = noise(splits[3], (SECTIONS, TOKENS, D), 0.125, 0.75, ((0, 8), (1, 4)))
    fresh_act = noise(splits[4], (TICKS, TOKENS, D), 1.0, 6.0, ((1, 4),))
    loss_cot = noise(splits[5], (TICKS, TOKENS, D), 0.125, 0.75, ((1, 4),))
    stash_act = noise(splits[6], (SECTIONS, TICKS, TOKENS, D), 1.0, 6.0, ((0, 8), (2, 4)))
    stash_act_tan = noise(splits[7], (SECTIONS, TICKS, TOKENS, D), 1.0, 6.0, ((0, 8), (2, 4)))
    norm_gain = jnp.clip(1.0 + 0.15 * jax.random.normal(splits[8], (SECTIONS, D), jnp.float32), 0.25, 1.75).astype(jnp.bfloat16)
    up_weight = noise(splits[9], (SECTIONS, D, FF), D ** -0.5, 0.125, ((0, 8), (2, 4)))
    down_weight = noise(splits[10], (SECTIONS, FF, D), FF ** -0.5, 0.09375, ((0, 8), (1, 4)))
    up_dir = noise(splits[11], (SECTIONS, D, FF), D ** -0.5, 0.125, ((0, 8), (2, 4)))
    down_dir = noise(splits[12], (SECTIONS, FF, D), FF ** -0.5, 0.09375, ((0, 8), (1, 4)))
    return dict(carry_act=carry_act, carry_act_tan=carry_act_tan, carry_adj=carry_adj, carry_adj_tan=carry_adj_tan, fresh_act=fresh_act, loss_cot=loss_cot, stash_act=stash_act, stash_act_tan=stash_act_tan, norm_gain=norm_gain, up_weight=up_weight, down_weight=down_weight, up_dir=up_dir, down_dir=down_dir)


sqrt_two_over_pi = 0.7978845608028654
cubic_coef = 0.044715
norm_eps = 1e-06

def gelu_parts(linear):
    inner_arg = sqrt_two_over_pi * (linear + cubic_coef * linear * linear * linear)
    first_slope = sqrt_two_over_pi * (1.0 + 3.0 * cubic_coef * linear * linear)
    second_slope = 6.0 * sqrt_two_over_pi * cubic_coef * linear
    tanh_value = jnp.tanh(inner_arg)
    sech_square = 1.0 - tanh_value * tanh_value
    gelu_value = 0.5 * linear * (1.0 + tanh_value)
    gelu_first = 0.5 * (1.0 + tanh_value) + 0.5 * linear * sech_square * first_slope
    gelu_second = sech_square * (first_slope - linear * tanh_value * first_slope * first_slope + 0.5 * linear * second_slope)
    return (gelu_value, gelu_first, gelu_second)

def matrix_product(left, right):
    return jnp.dot(left, right, preferred_element_type=jnp.float32)

def product_last(left, right):
    return lax.dot_general(left, right, (((1,), (1,)), ((), ())), preferred_element_type=jnp.float32)

def product_first(left, right):
    return lax.dot_general(left, right, (((0,), (0,)), ((), ())), preferred_element_type=jnp.float32)

def norm_stats(rows, rows_tan):
    values = rows.astype(jnp.float32)
    values_tan = rows_tan.astype(jnp.float32)
    inverse = lax.rsqrt(lax.optimization_barrier(jnp.mean(values * values, axis=-1, keepdims=True)) + norm_eps)
    inverse_tan = -(inverse * inverse * inverse) * lax.optimization_barrier(jnp.mean(values * values_tan, axis=-1, keepdims=True))
    return (values, values_tan, inverse, inverse_tan)

def norm_rows(rows, rows_tan, gain_row):
    values, values_tan, inverse, inverse_tan = norm_stats(rows, rows_tan)
    gain_wide = gain_row.astype(jnp.float32)
    normed = (values * inverse * gain_wide).astype(jnp.bfloat16)
    normed_tan = ((values_tan * inverse + values * inverse_tan) * gain_wide).astype(jnp.bfloat16)
    return (normed, normed_tan)

def norm_back(rows, rows_tan, gain_row, arriving, arriving_tan, summed, summed_tan):
    values, values_tan, inverse, inverse_tan = norm_stats(rows, rows_tan)
    gain_wide = gain_row.astype(jnp.float32)
    weighted = summed * gain_wide
    weighted_tan = summed_tan * gain_wide
    moment = lax.optimization_barrier(jnp.mean(values * weighted, axis=-1, keepdims=True))
    moment_tan = lax.optimization_barrier(jnp.mean(values_tan * weighted + values * weighted_tan, axis=-1, keepdims=True))
    inverse_cube = inverse * inverse * inverse
    returned = arriving.astype(jnp.float32) + inverse * weighted - inverse_cube * values * moment
    returned_tan = arriving_tan.astype(jnp.float32) + inverse_tan * weighted + inverse * weighted_tan - 3.0 * inverse * inverse * inverse_tan * values * moment - inverse_cube * values_tan * moment - inverse_cube * values * moment_tan
    return (returned.astype(jnp.bfloat16), returned_tan.astype(jnp.bfloat16))

def branch_forward(normed, normed_tan, up_local, down_local, up_direction, down_direction):
    linear = matrix_product(normed, up_local)
    linear_tan = matrix_product(normed_tan, up_local) + matrix_product(normed, up_direction)
    gelu_value, gelu_first, gelu_second = gelu_parts(linear)
    hidden = gelu_value.astype(jnp.bfloat16)
    hidden_tan = (gelu_first * linear_tan).astype(jnp.bfloat16)
    partial_value = matrix_product(hidden, down_local)
    partial_tan = matrix_product(hidden_tan, down_local) + matrix_product(hidden, down_direction)
    return (partial_value, partial_tan)

def branch_backward(stash_normed, stash_normed_tan, adjoint_all, adjoint_all_tan, up_local, down_local, up_direction, down_direction):
    linear = matrix_product(stash_normed, up_local)
    linear_tan = matrix_product(stash_normed_tan, up_local) + matrix_product(stash_normed, up_direction)
    gelu_value, gelu_first, gelu_second = gelu_parts(linear)
    hidden = gelu_value.astype(jnp.bfloat16)
    hidden_tan = (gelu_first * linear_tan).astype(jnp.bfloat16)
    upstream = product_last(adjoint_all, down_local)
    upstream_tan = product_last(adjoint_all_tan, down_local) + product_last(adjoint_all, down_direction)
    deltas = (upstream * gelu_first).astype(jnp.bfloat16)
    deltas_tan = (upstream_tan * gelu_first + upstream * gelu_second * linear_tan).astype(jnp.bfloat16)
    curvature_down = product_first(hidden_tan, adjoint_all) + product_first(hidden, adjoint_all_tan)
    curvature_up = product_first(stash_normed_tan, deltas) + product_first(stash_normed, deltas_tan)
    partial_value = product_last(deltas, up_local)
    partial_tan = product_last(deltas_tan, up_local) + product_last(deltas, up_direction)
    return (partial_value, partial_tan, curvature_up, curvature_down)

def sum_slices(parts):
    rounded = lax.optimization_barrier(parts.astype(jnp.bfloat16)).astype(jnp.float32)
    return lax.optimization_barrier(jnp.sum(rounded, axis=0))

def one_section(packed):
    input_rows, input_tan, arriving, arriving_tan, stash_rows, stash_tan, gain_row, up_section, down_section, up_section_dir, down_section_dir = packed
    width = FF // N_DP
    up_sliced = jnp.moveaxis(up_section.reshape(D, N_DP, width), 1, 0)
    up_dir_sliced = jnp.moveaxis(up_section_dir.reshape(D, N_DP, width), 1, 0)
    down_sliced = down_section.reshape(N_DP, width, D)
    down_dir_sliced = down_section_dir.reshape(N_DP, width, D)
    normed, normed_tan = norm_rows(input_rows, input_tan, gain_row)

    def forward_slice(weights):
        return branch_forward(normed, normed_tan, weights[0], weights[1], weights[2], weights[3])
    partials = lax.map(forward_slice, (up_sliced, down_sliced, up_dir_sliced, down_dir_sliced))
    new_act = (input_rows.astype(jnp.float32) + sum_slices(partials[0])).astype(jnp.bfloat16)
    new_act_tan = (input_tan.astype(jnp.float32) + sum_slices(partials[1])).astype(jnp.bfloat16)
    stash_normed, stash_normed_tan = norm_rows(stash_rows, stash_tan, gain_row)

    def backward_slice(weights):
        return branch_backward(stash_normed, stash_normed_tan, arriving, arriving_tan, weights[0], weights[1], weights[2], weights[3])
    backs = lax.map(backward_slice, (up_sliced, down_sliced, up_dir_sliced, down_dir_sliced))
    summed = sum_slices(backs[0])
    summed_tan = sum_slices(backs[1])
    curvature_up = jnp.moveaxis(backs[2], 0, 1).reshape(D, FF)
    curvature_down = backs[3].reshape(FF, D)
    new_adj, new_adj_tan = norm_back(stash_rows, stash_tan, gain_row, arriving, arriving_tan, summed, summed_tan)
    return (new_act, new_act_tan, new_adj, new_adj_tan, curvature_up, curvature_down)

def reference(carry_act, carry_act_tan, carry_adj, carry_adj_tan, fresh_act, loss_cot, stash_act, stash_act_tan, norm_gain, up_weight, down_weight, up_dir, down_dir):
    activation, activation_tan = (carry_act, carry_act_tan)
    adjoint, adjoint_tan = (carry_adj, carry_adj_tan)
    total_up = jnp.zeros(up_weight.shape, jnp.float32)
    total_down = jnp.zeros(down_weight.shape, jnp.float32)
    for tick_index in range(TICKS):
        zero_rows = jnp.zeros_like(fresh_act[tick_index])
        input_rows = jnp.concatenate([fresh_act[tick_index][None], activation[:-1]], axis=0)
        input_tan = jnp.concatenate([zero_rows[None], activation_tan[:-1]], axis=0)
        arriving = jnp.concatenate([adjoint[1:], loss_cot[tick_index][None]], axis=0)
        arriving_tan = jnp.concatenate([adjoint_tan[1:], zero_rows[None]], axis=0)
        results = lax.map(one_section, (input_rows, input_tan, arriving, arriving_tan, stash_act[:, tick_index], stash_act_tan[:, tick_index], norm_gain, up_weight, down_weight, up_dir, down_dir))
        activation, activation_tan, adjoint, adjoint_tan = (results[0], results[1], results[2], results[3])
        total_up = total_up + results[4]
        total_down = total_down + results[5]
    return (activation, activation_tan, adjoint, adjoint_tan, total_up.astype(jnp.bfloat16), total_down.astype(jnp.bfloat16))
```

```python
import jax
import jax.numpy as jnp
from jax import lax
from jax.experimental import pallas as pl
from jax.experimental.pallas import tpu as pltpu
from jax.sharding import PartitionSpec as P

TICKS = 2


sqrt_two_over_pi = 0.7978845608028654
cubic_coef = 0.044715
norm_eps = 1e-06

bf16 = jnp.bfloat16
f32 = jnp.float32
VM = pl.BlockSpec(memory_space=pltpu.VMEM)


def params(mib):
    return pltpu.CompilerParams(vmem_limit_bytes=mib * 2**20)


def passed_along(value, axis, steps):
    count = lax.axis_size(axis)
    leading, last = (max(0, -steps), min(count, count - steps))
    return lax.ppermute(value, axis, [(source, source + steps) for source in range(leading, last)])


def swapped(value, bit):
    count = lax.axis_size("dp")
    return lax.ppermute(value, "dp", [(source, source ^ bit) for source in range(count)])


def dp_bits():
    count = lax.axis_size("dp")
    bits = []
    bit = count // 2
    while bit:
        bits.append(bit)
        bit //= 2
    return bits


def gather_blocks(block):
    blocks = [block]
    for bit in dp_bits():
        blocks = blocks + [swapped(b, bit) for b in blocks]
    return blocks


def gelu_parts(linear):
    inner_arg = sqrt_two_over_pi * (linear + cubic_coef * linear * linear * linear)
    first_slope = sqrt_two_over_pi * (1.0 + 3.0 * cubic_coef * linear * linear)
    second_slope = 6.0 * sqrt_two_over_pi * cubic_coef * linear
    tanh_value = jnp.tanh(inner_arg)
    sech_square = 1.0 - tanh_value * tanh_value
    gelu_value = 0.5 * linear * (1.0 + tanh_value)
    gelu_first = 0.5 * (1.0 + tanh_value) + 0.5 * linear * sech_square * first_slope
    gelu_second = sech_square * (
        first_slope - linear * tanh_value * first_slope * first_slope + 0.5 * linear * second_slope
    )
    return (gelu_value, gelu_first, gelu_second)


def matrix_product(left, right):
    return jnp.dot(left, right, preferred_element_type=f32)


def product_last(left, right):
    return lax.dot_general(left, right, (((1,), (1,)), ((), ())), preferred_element_type=f32)


def product_first(left, right):
    return lax.dot_general(left, right, (((0,), (0,)), ((), ())), preferred_element_type=f32)


def norm_stats(values, values_tan):
    inverse = lax.rsqrt(jnp.mean(values * values, axis=-1, keepdims=True) + norm_eps)
    inverse_tan = -(inverse * inverse * inverse) * jnp.mean(
        values * values_tan, axis=-1, keepdims=True
    )
    return (inverse, inverse_tan)


def norm_rows(values, values_tan, gain_wide):
    inverse, inverse_tan = norm_stats(values, values_tan)
    normed = values * inverse * gain_wide
    normed_tan = (values_tan * inverse + values * inverse_tan) * gain_wide
    return (normed, normed_tan)


def pick(blocks, index, rows):
    return jnp.concatenate(
        [b[index * rows : (index + 1) * rows, :].astype(f32) for b in blocks], axis=0
    )


def stash_kernel(count, rows):
    def body(*refs):
        blocks = refs[:count]
        gain_ref, up_ref, dup_ref = refs[count : count + 3]
        m_ref, q_ref, slope_ref, bend_ref = refs[count + 3 :]
        gain_wide = gain_ref[...].astype(f32)
        tokens = count * rows
        for tick in range(TICKS):
            normed, normed_tan = norm_rows(
                pick(blocks, 2 * tick, rows), pick(blocks, 2 * tick + 1, rows), gain_wide
            )
            base = 2 * tick * tokens
            m_ref[base : base + tokens, :] = normed_tan.astype(bf16)
            m_ref[base + tokens : base + 2 * tokens, :] = normed.astype(bf16)
        both = matrix_product(m_ref[...], up_ref[...])
        plain = jnp.concatenate(
            [m_ref[(2 * t + 1) * tokens : (2 * t + 2) * tokens, :] for t in range(TICKS)], axis=0
        )
        side = matrix_product(plain, dup_ref[...])
        for tick in range(TICKS):
            base = 2 * tick * tokens
            linear = both[base + tokens : base + 2 * tokens]
            linear_tan = both[base : base + tokens] + side[tick * tokens : (tick + 1) * tokens]
            value, first, second = gelu_parts(linear)
            q_ref[base : base + tokens, :] = (first * linear_tan).astype(bf16)
            q_ref[base + tokens : base + 2 * tokens, :] = value.astype(bf16)
            slope_ref[tick * tokens : (tick + 1) * tokens, :] = first
            bend_ref[tick * tokens : (tick + 1) * tokens, :] = second * linear_tan

    return body


def tick_kernel(count, rows, tick):
    tokens = count * rows
    half = count // 2

    def body(*refs):
        blocks = refs[:count]
        gain_ref, up_ref, down_ref, dup_ref, ddown_ref, slope_ref, bend_ref = refs[
            count : count + 7
        ]
        keep_ref, send_ref, z_ref, adj_ref = refs[count + 7 :]
        gain_wide = gain_ref[...].astype(f32)
        normed, normed_tan = norm_rows(pick(blocks, 0, rows), pick(blocks, 1, rows), gain_wide)
        pair = jnp.concatenate([normed, normed_tan], axis=0).astype(bf16)
        both = matrix_product(pair, up_ref[...])
        linear = both[:tokens]
        linear_tan = both[tokens:] + matrix_product(pair[:tokens], dup_ref[...])
        value, first, _ = gelu_parts(linear)
        hidden = jnp.concatenate([value, first * linear_tan], axis=0).astype(bf16)
        p_both = matrix_product(hidden, down_ref[...])
        p_tan = p_both[tokens:] + matrix_product(hidden[:tokens], ddown_ref[...])
        adj = jnp.concatenate([pick(blocks, 2, rows), pick(blocks, 3, rows)], axis=0).astype(bf16)
        adj_ref[...] = adj
        e_both = product_last(adj, down_ref[...])
        e_tan = e_both[tokens:] + product_last(adj[:tokens], ddown_ref[...])
        upstream = e_both[:tokens]
        span = slice(tick * tokens, (tick + 1) * tokens)
        slope = slope_ref[span, :]
        z_pair = jnp.concatenate(
            [upstream * slope, e_tan * slope + upstream * bend_ref[span, :]], axis=0
        ).astype(bf16)
        z_ref[...] = z_pair
        t_both = product_last(z_pair, up_ref[...])
        t_tan = t_both[tokens:] + product_last(z_pair[:tokens], dup_ref[...])
        parts = (p_both[:tokens], p_tan, t_both[:tokens], t_tan)
        for k in range(count):
            for a in range(4):
                piece = parts[a][k * rows : (k + 1) * rows]
                if k < half:
                    at = (4 * k + a) * rows
                    keep_ref[at : at + rows, :] = piece
                else:
                    at = (4 * (k - half) + a) * rows
                    send_ref[at : at + rows, :] = piece.astype(bf16)

    return body


def add_body(keep_ref, got_ref, low_ref, high_ref):
    half = keep_ref.shape[0] // 2
    low_ref[...] = keep_ref[:half, :] + got_ref[:half, :].astype(f32)
    high_ref[...] = (keep_ref[half:, :] + got_ref[half:, :].astype(f32)).astype(bf16)


def finish_kernel(rows):
    def body(keep_ref, got_ref, own_ref, stash_ref, stash_tan_ref, gain_ref, fwd_ref, bwd_ref):
        total = keep_ref[...] + got_ref[...].astype(f32)
        own = own_ref[...].astype(f32)
        values = stash_ref[...].astype(f32)
        values_tan = stash_tan_ref[...].astype(f32)
        gain_wide = gain_ref[...].astype(f32)
        fwd_ref[...] = (own[: 2 * rows] + total[: 2 * rows]).astype(bf16)
        inverse, inverse_tan = norm_stats(values, values_tan)
        weighted = total[2 * rows : 3 * rows] * gain_wide
        weighted_tan = total[3 * rows :] * gain_wide
        moment = jnp.mean(values * weighted, axis=-1, keepdims=True)
        moment_tan = jnp.mean(
            values_tan * weighted + values * weighted_tan, axis=-1, keepdims=True
        )
        inverse_cube = inverse * inverse * inverse
        returned = own[2 * rows : 3 * rows] + inverse * weighted - inverse_cube * values * moment
        returned_tan = (
            own[3 * rows :]
            + inverse_tan * weighted
            + inverse * weighted_tan
            - 3.0 * inverse * inverse * inverse_tan * values * moment
            - inverse_cube * values_tan * moment
            - inverse_cube * values * moment_tan
        )
        bwd_ref[:rows, :] = returned.astype(bf16)
        bwd_ref[rows:, :] = returned_tan.astype(bf16)

    return body


def curvature_body(m_ref, z_refs, q_ref, adj_refs, up_ref, down_ref):
    z_all = jnp.concatenate([r[...] for r in z_refs], axis=0)
    adj_all = jnp.concatenate([r[...] for r in adj_refs], axis=0)
    up_ref[...] = product_first(m_ref[...], z_all).astype(bf16)
    down_ref[...] = product_first(q_ref[...], adj_all).astype(bf16)


def call(body, outs, mib, *operands):
    return pl.pallas_call(
        body,
        in_specs=[VM] * len(operands),
        out_specs=[VM] * len(outs),
        out_shape=[jax.ShapeDtypeStruct(s, d) for s, d in outs],
        compiler_params=params(mib),
    )(*operands)


def shards(
    carry_act,
    carry_act_tan,
    carry_adj,
    carry_adj_tan,
    fresh_act,
    loss_cot,
    stash_act,
    stash_act_tan,
    norm_gain,
    up_weight,
    down_weight,
    up_dir,
    down_dir,
):
    section_index = lax.axis_index("section")
    section_count = lax.axis_size("section")
    count = lax.axis_size("dp")
    at_first = section_index == 0
    at_last = section_index == section_count - 1
    up_local = up_weight[0]
    down_local = down_weight[0]
    up_direction = up_dir[0]
    down_direction = down_dir[0]
    rows, width = carry_act.shape[1:]
    hidden = up_local.shape[1]
    tokens = count * rows

    def arrival(moved_forward, moved_backward, tick):
        zero_rows = jnp.zeros((rows, width), bf16)
        edge = (
            (at_first, fresh_act[tick], moved_forward[:rows]),
            (at_first, zero_rows, moved_forward[rows:]),
            (at_last, loss_cot[tick], moved_backward[:rows]),
            (at_last, zero_rows, moved_backward[rows:]),
        )
        return jnp.concatenate([jnp.where(*e) for e in edge], axis=0)

    forward = jnp.concatenate([carry_act[0], carry_act_tan[0]], axis=0)
    backward = jnp.concatenate([carry_adj[0], carry_adj_tan[0]], axis=0)
    moved_forward = passed_along(forward, "section", 1)
    moved_backward = passed_along(backward, "section", -1)

    stash_own = jnp.concatenate(
        [x for t in range(TICKS) for x in (stash_act[0, t], stash_act_tan[0, t])], axis=0
    )
    stash_blocks = gather_blocks(stash_own)
    pairs = 2 * TICKS * tokens
    m_all, q_all, slope, bend = call(
        stash_kernel(count, rows),
        [
            ((pairs, width), bf16),
            ((pairs, hidden), bf16),
            ((TICKS * tokens, hidden), f32),
            ((TICKS * tokens, hidden), f32),
        ],
        16,
        *stash_blocks,
        norm_gain,
        up_local,
        up_direction,
    )
    z_list, adj_list = [], []
    for tick in range(TICKS):
        own = arrival(moved_forward, moved_backward, tick)
        blocks = gather_blocks(own)
        half = count // 2
        keep, send, z_pair, adj = call(
            tick_kernel(count, rows, tick),
            [
                ((half * 4 * rows, width), f32),
                ((half * 4 * rows, width), bf16),
                ((2 * tokens, hidden), bf16),
                ((2 * tokens, width), bf16),
            ],
            16,
            *blocks,
            norm_gain,
            up_local,
            down_local,
            up_direction,
            down_direction,
            slope,
            bend,
        )
        z_list.append(z_pair)
        adj_list.append(adj)
        bits = dp_bits()[::-1]
        for bit in bits[:-1]:
            got = swapped(send, bit)
            part = keep.shape[0] // 2
            keep, send = call(
                add_body, [((part, width), f32), ((part, width), bf16)], 8, keep, got
            )
        got = swapped(send, bits[-1])
        forward, backward = call(
            finish_kernel(rows),
            [((2 * rows, width), bf16), ((2 * rows, width), bf16)],
            8,
            keep,
            got,
            own,
            stash_act[0, tick],
            stash_act_tan[0, tick],
            norm_gain,
        )
        if tick + 1 < TICKS:
            moved_forward = passed_along(forward, "section", 1)
            moved_backward = passed_along(backward, "section", -1)

    def curvature(m_ref, *refs):
        curvature_body(
            m_ref, refs[:TICKS], refs[TICKS], refs[TICKS + 1 : 2 * TICKS + 1], *refs[2 * TICKS + 1 :]
        )

    steps = next(
        n for n in range(width // 256, 0, -1)
        if n == 1 or (width % (128 * n) == 0 and hidden % (128 * n) == 0)
    )
    lead = hidden // steps
    whole = lambda shape: pl.BlockSpec(shape, lambda i: (0, 0))
    total_up, total_down = pl.pallas_call(
        curvature,
        grid=(steps,),
        in_specs=[pl.BlockSpec((pairs, width // steps), lambda i: (0, i))]
        + [whole(z.shape) for z in z_list]
        + [pl.BlockSpec((pairs, lead), lambda i: (0, i))]
        + [whole(a.shape) for a in adj_list],
        out_specs=[
            pl.BlockSpec((width // steps, hidden), lambda i: (i, 0)),
            pl.BlockSpec((lead, width), lambda i: (i, 0)),
        ],
        out_shape=[
            jax.ShapeDtypeStruct((width, hidden), bf16),
            jax.ShapeDtypeStruct((hidden, width), bf16),
        ],
        compiler_params=params(24),
    )(m_all, *z_list, q_all, *adj_list)
    return (
        forward[:rows][None],
        forward[rows:][None],
        backward[:rows][None],
        backward[rows:][None],
        total_up[None],
        total_down[None],
    )


def solution(mesh):
    in_specs = (
        P("section", "dp", None),
        P("section", "dp", None),
        P("section", "dp", None),
        P("section", "dp", None),
        P(None, "dp", None),
        P(None, "dp", None),
        P("section", None, "dp", None),
        P("section", None, "dp", None),
        P("section", None),
        P("section", None, "dp"),
        P("section", "dp", None),
        P("section", None, "dp"),
        P("section", "dp", None),
    )
    out_specs = (
        P("section", "dp", None),
        P("section", "dp", None),
        P("section", "dp", None),
        P("section", "dp", None),
        P("section", None, "dp"),
        P("section", "dp", None),
    )
    return jax.shard_map(shards, mesh=mesh, in_specs=in_specs, out_specs=out_specs, check_vma=False)
```

```python
import jax
import jax.numpy as jnp
from jax import lax
from jax.experimental import pallas as pl
from jax.experimental.pallas import tpu as pltpu
from jax.sharding import PartitionSpec as P

TICKS = 2


sqrt_two_over_pi = 0.7978845608028654
cubic_coef = 0.044715
norm_eps = 1e-06

bf16 = jnp.bfloat16
f32 = jnp.float32
VM = pl.BlockSpec(memory_space=pltpu.VMEM)
HBM = pl.BlockSpec(memory_space=pltpu.HBM)


def params(mib):
    return pltpu.CompilerParams(vmem_limit_bytes=mib * 2**20)


def passed_along(value, axis, steps):
    count = lax.axis_size(axis)
    leading, last = (max(0, -steps), min(count, count - steps))
    return lax.ppermute(value, axis, [(source, source + steps) for source in range(leading, last)])


def swapped(value, bit):
    count = lax.axis_size("dp")
    return lax.ppermute(value, "dp", [(source, source ^ bit) for source in range(count)])


def dp_bits():
    count = lax.axis_size("dp")
    bits = []
    bit = count // 2
    while bit:
        bits.append(bit)
        bit //= 2
    return bits


def gather_blocks(block, bits):
    blocks = [block]
    for bit in bits:
        blocks = blocks + [swapped(b, bit) for b in blocks]
    return blocks


def parity_moved(value):
    sections, count = (lax.axis_size("section"), lax.axis_size("dp"))
    pairs = []
    for section in range(sections):
        for member in range(count):
            target = section + (1 if member % 2 == 0 else -1)
            if 0 <= target < sections:
                pairs.append((section * count + member, target * count + member))
    return lax.ppermute(value, ("section", "dp"), pairs)


def gelu_parts(linear):
    inner_arg = sqrt_two_over_pi * (linear + cubic_coef * linear * linear * linear)
    first_slope = sqrt_two_over_pi * (1.0 + 3.0 * cubic_coef * linear * linear)
    second_slope = 6.0 * sqrt_two_over_pi * cubic_coef * linear
    tanh_value = jnp.tanh(inner_arg)
    sech_square = 1.0 - tanh_value * tanh_value
    gelu_value = 0.5 * linear * (1.0 + tanh_value)
    gelu_first = 0.5 * (1.0 + tanh_value) + 0.5 * linear * sech_square * first_slope
    gelu_second = sech_square * (
        first_slope - linear * tanh_value * first_slope * first_slope + 0.5 * linear * second_slope
    )
    return (gelu_value, gelu_first, gelu_second)


def matrix_product(left, right):
    return jnp.dot(left, right, preferred_element_type=f32)


def product_last(left, right):
    return lax.dot_general(left, right, (((1,), (1,)), ((), ())), preferred_element_type=f32)


def product_first(left, right):
    return lax.dot_general(left, right, (((0,), (0,)), ((), ())), preferred_element_type=f32)


def norm_stats(values, values_tan):
    inverse = lax.rsqrt(jnp.mean(values * values, axis=-1, keepdims=True) + norm_eps)
    inverse_tan = -(inverse * inverse * inverse) * jnp.mean(
        values * values_tan, axis=-1, keepdims=True
    )
    return (inverse, inverse_tan)


def norm_rows(values, values_tan, gain_wide):
    inverse, inverse_tan = norm_stats(values, values_tan)
    normed = values * inverse * gain_wide
    normed_tan = (values_tan * inverse + values * inverse_tan) * gain_wide
    return (normed, normed_tan)


def piece(block, index, rows):
    return block[index * rows : (index + 1) * rows, :].astype(f32)


def pick(blocks, index, rows):
    return jnp.concatenate([piece(b, index, rows) for b in blocks], axis=0)


def pack_kernel(rows):
    later = TICKS - 1

    def body(*refs):
        act, act_tan, adj, adj_tan, fresh, loss, stash, stash_tan, gain = refs[:9]
        fwd, bwd, store, edge, gain_out = refs[9:14]
        late, sems = refs[14:]
        pairs = [
            (act.at[0], fwd.at[pl.ds(0, rows)]),
            (act_tan.at[0], fwd.at[pl.ds(rows, rows)]),
            (adj.at[0], bwd.at[pl.ds(0, rows)]),
            (adj_tan.at[0], bwd.at[pl.ds(rows, rows)]),
            (fresh.at[0], edge.at[pl.ds(0, rows)]),
            (loss.at[0], edge.at[pl.ds(rows, rows)]),
            (gain, gain_out),
        ]
        for tick in range(TICKS):
            pairs.append((stash.at[0, tick], store.at[pl.ds(2 * tick * rows, rows)]))
            pairs.append((stash_tan.at[0, tick], store.at[pl.ds((2 * tick + 1) * rows, rows)]))
        for tick in range(1, TICKS):
            pairs.append((fresh.at[tick], late.at[pl.ds(2 * (tick - 1) * rows, rows)]))
            pairs.append((loss.at[tick], late.at[pl.ds((2 * tick - 1) * rows, rows)]))
        copies = [pltpu.make_async_copy(a, b, sems.at[i]) for i, (a, b) in enumerate(pairs)]
        for copy in copies:
            copy.start()
        for copy in copies:
            copy.wait()
        section = lax.axis_index("section")
        at_first = section == 0
        at_last = section == lax.axis_size("section") - 1
        for k in range(2 * later):
            rows_late = late[k * rows : (k + 1) * rows, :].astype(f32)
            masked = jnp.where(at_first if k % 2 == 0 else at_last, rows_late, 0.0)
            base = (2 * TICKS + k) * rows
            store[base : base + rows, :] = masked.astype(bf16)

    return body


def arrive_kernel(rows):
    def body(fwd_ref, bwd_ref, edge_ref, token_ref, own_ref):
        section = lax.axis_index("section")
        at_first = section == 0
        at_last = section == lax.axis_size("section") - 1
        own_ref[:rows, :] = jnp.where(
            at_first, piece(edge_ref, 0, rows), piece(fwd_ref, 0, rows)
        ).astype(bf16)
        own_ref[rows : 2 * rows, :] = fwd_ref[rows:, :]
        own_ref[2 * rows : 3 * rows, :] = jnp.where(
            at_last, piece(edge_ref, 1, rows), piece(bwd_ref, 0, rows)
        ).astype(bf16)
        own_ref[3 * rows :, :] = bwd_ref[rows:, :]

    return body


def chunk_rows(total, limit):
    sizes = [c for c in range(128, limit + 1, 128) if total % c == 0]
    return sizes[-1] if sizes else total


def start_all(copies):
    for copy in copies:
        copy.start()


def load_down_kernel(step):
    def body(down_hbm, ddown_hbm, down_ref, down_t_ref, ddown_ref, ddown_t_ref, token, sems):
        token[...] = jnp.zeros_like(token)
        steps = down_hbm.shape[0] // step
        loads = ((down_hbm, down_ref, down_t_ref), (ddown_hbm, ddown_ref, ddown_t_ref))

        def copies(i):
            span = pl.ds(pl.multiple_of(i * step, step), step)
            return [
                pltpu.make_async_copy(src.at[span], dst.at[span], sems.at[2 * i + k])
                for k, (src, dst, _) in enumerate(loads)
            ]

        lax.fori_loop(0, steps, lambda i, c: start_all(copies(i)), None)

        def work(i, carry):
            span = pl.ds(pl.multiple_of(i * step, step), step)
            for copy, (_, dst, flip) in zip(copies(i), loads):
                copy.wait()
                flip[:, span] = dst[span, :].T

        lax.fori_loop(0, steps, work, None)

    return body


def stash_kernel(count, rows, step):
    tokens = count * rows

    def body(*refs):
        blocks = refs[:count]
        gain_ref, up_hbm, dup_hbm = refs[count : count + 3]
        (
            m_ref,
            q_ref,
            slope_ref,
            bend_ref,
            up_ref,
            dup_ref,
            stack,
            plain,
            both,
            side,
            sems,
        ) = refs[count + 3 :]
        steps = up_hbm.shape[0] // step
        loads = ((up_hbm, up_ref), (dup_hbm, dup_ref))

        def copies(i):
            span = pl.ds(pl.multiple_of(i * step, step), step)
            return [
                pltpu.make_async_copy(src.at[span], dst.at[span], sems.at[2 * i + k])
                for k, (src, dst) in enumerate(loads)
            ]

        lax.fori_loop(0, steps, lambda i, c: start_all(copies(i)), None)
        gain_wide = gain_ref[...].astype(f32)
        for tick in range(TICKS):
            normed, normed_tan = norm_rows(
                pick(blocks, 2 * tick, rows), pick(blocks, 2 * tick + 1, rows), gain_wide
            )
            base = 2 * tick * tokens
            stack[base : base + tokens, :] = normed_tan.astype(bf16)
            stack[base + tokens : base + 2 * tokens, :] = normed.astype(bf16)
            plain[tick * tokens : (tick + 1) * tokens, :] = normed.astype(bf16)
        m_ref[...] = stack[...].T
        both[...] = jnp.zeros_like(both)
        side[...] = jnp.zeros_like(side)

        def work(i, carry):
            span = pl.ds(pl.multiple_of(i * step, step), step)
            sides = zip(copies(i), loads, ((stack, both), (plain, side)))
            for copy, (_, dst), (left, total) in sides:
                copy.wait()
                total[...] += matrix_product(left[:, span], dst[span, :])

        lax.fori_loop(0, steps, work, None)
        for tick in range(TICKS):
            base = 2 * tick * tokens
            linear = both[base + tokens : base + 2 * tokens, :]
            linear_tan = (
                both[base : base + tokens, :] + side[tick * tokens : (tick + 1) * tokens, :]
            )
            value, first, second = gelu_parts(linear)
            q_pair = jnp.concatenate([first * linear_tan, value], axis=0).astype(bf16)
            q_ref[:, base : base + 2 * tokens] = q_pair.T
            slope_ref[tick * tokens : (tick + 1) * tokens, :] = first
            bend_ref[tick * tokens : (tick + 1) * tokens, :] = second * linear_tan

    return body


def tick_kernel(count, rows, tick):
    tokens = count * rows
    half = count // 2
    n_in = count if tick == 0 else 2 * count

    def body(*refs):
        blocks = refs[:n_in]
        (
            gain_ref,
            up_ref,
            dup_ref,
            down_ref,
            down_t_ref,
            ddown_ref,
            ddown_t_ref,
            slope_ref,
            bend_ref,
        ) = refs[n_in : n_in + 9]
        outs = refs[n_in + 9 : -2]
        pair_ref, hid_ref = refs[-2:]
        keep_ref, send_ref, z_ref, adj_ref = outs[:4]
        even = (lax.axis_index("dp") & 1) == 0
        gain_wide = gain_ref[...].astype(f32)
        if tick == 0:
            values = [pick(blocks, a, rows) for a in range(4)]
        else:
            mine, theirs, edges = (blocks[:half], blocks[half:count], blocks[count:])
            values = []
            for chain in range(2):
                for a in range(2):
                    here = [piece(u, 2 * b + a, rows) for b in (0, 1) for u in mine]
                    there = [piece(u, 2 * b + a, rows) for b in (1, 0) for u in theirs]
                    here = jnp.concatenate(here, axis=0)
                    there = jnp.concatenate(there, axis=0)
                    first, second = (here, there) if chain == 0 else (there, here)
                    value = jnp.where(even, first, second)
                    if a == 0:
                        value = value + pick(edges, 2 * TICKS + 2 * (tick - 1) + chain, rows)
                    values.append(value)
            if len(outs) > 4:
                for a in range(4):
                    outs[4][a * rows : (a + 1) * rows, :] = values[a][:rows].astype(bf16)
        normed, normed_tan = norm_rows(values[0], values[1], gain_wide)
        pair_ref[:tokens, :] = normed.astype(bf16)
        pair_ref[tokens:, :] = normed_tan.astype(bf16)
        adj_ref[:tokens, :] = values[2].astype(bf16)
        adj_ref[tokens:, :] = values[3].astype(bf16)
        hidden, width = up_ref.shape[1], up_ref.shape[0]
        size = 384 if hidden % 384 == 0 else hidden
        base = tick * tokens

        def inner(i, carry):
            at = i * size if hidden % size == 0 else jnp.minimum(i * size, hidden - size)
            span = pl.ds(pl.multiple_of(at, 128) if size != hidden else 0, size)
            both = matrix_product(pair_ref[...], up_ref[:, span])
            side = matrix_product(pair_ref[:tokens, :], dup_ref[:, span])
            e_both = matrix_product(adj_ref[...], down_t_ref[:, span])
            e_side = matrix_product(adj_ref[:tokens, :], ddown_t_ref[:, span])
            value, first, _ = gelu_parts(both[:tokens])
            hid_ref[:tokens, span] = value.astype(bf16)
            hid_ref[tokens:, span] = (first * (both[tokens:] + side)).astype(bf16)
            upstream = e_both[:tokens]
            slope = slope_ref[base : base + tokens, span]
            bend = bend_ref[base : base + tokens, span]
            z_ref[:tokens, span] = (upstream * slope).astype(bf16)
            z_ref[tokens:, span] = ((e_both[tokens:] + e_side) * slope + upstream * bend).astype(
                bf16
            )

        lax.fori_loop(0, -(-hidden // size), inner, None)
        size_out = 1152 if width % 1152 == 0 else width
        order = [k for j in range(half) for k in (j, j + half)]

        def outer(i, carry):
            span = pl.ds(pl.multiple_of(i * size_out, size_out), size_out)
            p_both = matrix_product(hid_ref[...], down_ref[:, span])
            p_side = matrix_product(hid_ref[:tokens, :], ddown_ref[:, span])
            t_both = product_last(z_ref[...], up_ref[span, :])
            t_side = product_last(z_ref[:tokens, :], dup_ref[span, :])
            parts = (
                p_both[:tokens],
                p_both[tokens:] + p_side,
                t_both[:tokens],
                t_both[tokens:] + t_side,
            )
            if tick + 1 == TICKS:
                for k in range(count):
                    for a in range(4):
                        part = parts[a][k * rows : (k + 1) * rows]
                        if k < half:
                            at = (4 * k + a) * rows
                            keep_ref[at : at + rows, span] = part
                        else:
                            at = (4 * (k - half) + a) * rows
                            send_ref[at : at + rows, span] = part.astype(bf16)
            else:
                kept = [jnp.where(even, parts[a], parts[a + 2]) for a in range(2)]
                sent = [jnp.where(even, parts[a + 2], parts[a]) for a in range(2)]
                for i, k in enumerate(order):
                    for a in range(2):
                        at = (2 * i + a) * rows
                        keep_ref[at : at + rows, span] = kept[a][k * rows : (k + 1) * rows]
                        at = (2 * (i ^ 1) + a) * rows
                        send_ref[at : at + rows, span] = sent[a][k * rows : (k + 1) * rows].astype(
                            bf16
                        )

        lax.fori_loop(0, width // size_out, outer, None)

    return body


def add_body(keep_ref, got_ref, low_ref, high_ref):
    half = keep_ref.shape[0] // 2
    low_ref[...] = keep_ref[:half, :] + got_ref[:half, :].astype(f32)
    high_ref[...] = (keep_ref[half:, :] + got_ref[half:, :].astype(f32)).astype(bf16)


def norm_back(values, values_tan, gain_wide, arriving, arriving_tan, summed, summed_tan):
    inverse, inverse_tan = norm_stats(values, values_tan)
    weighted = summed * gain_wide
    weighted_tan = summed_tan * gain_wide
    moment = jnp.mean(values * weighted, axis=-1, keepdims=True)
    moment_tan = jnp.mean(values_tan * weighted + values * weighted_tan, axis=-1, keepdims=True)
    inverse_cube = inverse * inverse * inverse
    returned = arriving + inverse * weighted - inverse_cube * values * moment
    returned_tan = (
        arriving_tan
        + inverse_tan * weighted
        + inverse * weighted_tan
        - 3.0 * inverse * inverse * inverse_tan * values * moment
        - inverse_cube * values_tan * moment
        - inverse_cube * values * moment_tan
    )
    return (returned, returned_tan)


def unit_kernel(rows, tick):
    def body(keep_ref, got_ref, own_ref, other_ref, stash_ref, stash_other_ref, gain_ref, out_ref):
        even = (lax.axis_index("dp") & 1) == 0
        total = keep_ref[...] + got_ref[...].astype(f32)
        sources = ((own_ref, stash_ref), (other_ref, stash_other_ref))

        @pl.when(even)
        def _():
            for b, (block, _) in enumerate(sources):
                for a in range(2):
                    at = (2 * b + a) * rows
                    out_ref[at : at + rows, :] = (
                        piece(block, a, rows) + total[at : at + rows]
                    ).astype(bf16)

        @pl.when(jnp.logical_not(even))
        def _():
            gain_wide = gain_ref[...].astype(f32)
            for b, (block, store) in enumerate(sources):
                at = 2 * b * rows
                returned = norm_back(
                    piece(store, 2 * tick, rows),
                    piece(store, 2 * tick + 1, rows),
                    gain_wide,
                    piece(block, 2, rows),
                    piece(block, 3, rows),
                    total[at : at + rows],
                    total[at + rows : at + 2 * rows],
                )
                for a in range(2):
                    out_ref[at + a * rows : at + (a + 1) * rows, :] = returned[a].astype(bf16)

    return body


def last_kernel(rows, tick):
    def body(keep_ref, got_ref, own_ref, stash_ref, gain_ref, *outs):
        total = keep_ref[...] + got_ref[...].astype(f32)
        parts = [total[a * rows : (a + 1) * rows] for a in range(4)]
        for a in range(2):
            outs[a][0] = (piece(own_ref, a, rows) + parts[a]).astype(bf16)
        returned = norm_back(
            piece(stash_ref, 2 * tick, rows),
            piece(stash_ref, 2 * tick + 1, rows),
            gain_ref[...].astype(f32),
            piece(own_ref, 2, rows),
            piece(own_ref, 3, rows),
            parts[2],
            parts[3],
        )
        for a in range(2):
            outs[2 + a][0] = returned[a].astype(bf16)

    return body


def curvature_kernel(steps):
    def body(*refs):
        m_ref, q_ref = refs[:2]
        z_refs, adj_refs = refs[2 : 2 + TICKS], refs[2 + TICKS : 2 + 2 * TICKS]
        up_hbm, down_hbm, up_ref, down_ref, sems = refs[2 + 2 * TICKS :]
        jobs = ((m_ref, z_refs, up_ref, up_hbm), (q_ref, adj_refs, down_ref, down_hbm))

        def copies(i):
            made = []
            for k, (_, _, ref, hbm) in enumerate(jobs):
                size = ref.shape[0] // steps
                span = pl.ds(pl.multiple_of(i * size, size), size)
                made.append(pltpu.make_async_copy(ref.at[span], hbm.at[span], sems.at[2 * i + k]))
            return made

        def work(i, carry):
            for copy, (left, rights, ref, _) in zip(copies(i), jobs):
                size = ref.shape[0] // steps
                span = pl.ds(pl.multiple_of(i * size, size), size)
                right = jnp.concatenate([r[...] for r in rights], axis=0)
                ref[span, :] = matrix_product(left[span, :], right).astype(bf16)
                copy.start()

        lax.fori_loop(0, steps, work, None)

        def finish(i, carry):
            for copy in copies(i):
                copy.wait()

        lax.fori_loop(0, steps, finish, None)

    return body


def call(body, outs, mib, *operands, specs=None, scratch=()):
    operands = [
        pltpu.with_memory_space_constraint(x, pltpu.HBM) if specs and specs[i] is HBM else x
        for i, x in enumerate(operands)
    ]
    return pl.pallas_call(
        body,
        in_specs=specs or [VM] * len(operands),
        out_specs=[VM] * len(outs),
        out_shape=[jax.ShapeDtypeStruct(*o) if isinstance(o, tuple) else o for o in outs],
        scratch_shapes=scratch,
        compiler_params=params(mib),
    )(*operands)


def shards(
    carry_act,
    carry_act_tan,
    carry_adj,
    carry_adj_tan,
    fresh_act,
    loss_cot,
    stash_act,
    stash_act_tan,
    norm_gain,
    up_weight,
    down_weight,
    up_dir,
    down_dir,
):
    count = lax.axis_size("dp")
    half = count // 2
    bits = dp_bits()
    rows, width = carry_act.shape[1:]
    hidden = up_weight.shape[2]
    tokens = count * rows
    pairs = 2 * TICKS * tokens
    late = 2 * (TICKS - 1) * rows
    grant = max(6, tokens // 5)

    n_copies = 7 + 2 * TICKS + 2 * (TICKS - 1)
    forward, backward, store, edge, gain = call(
        pack_kernel(rows),
        [
            ((2 * rows, width), bf16),
            ((2 * rows, width), bf16),
            ((2 * TICKS * rows + late, width), bf16),
            ((2 * rows, width), bf16),
            ((1, width), bf16),
        ],
        4,
        carry_act,
        carry_act_tan,
        carry_adj,
        carry_adj_tan,
        fresh_act,
        loss_cot,
        stash_act,
        stash_act_tan,
        norm_gain,
        specs=[HBM] * 9,
        scratch=[pltpu.VMEM((max(late, rows), width), bf16), pltpu.SemaphoreType.DMA((n_copies,))],
    )
    moved_forward = passed_along(forward, "section", 1)
    moved_backward = passed_along(backward, "section", -1)
    far = swapped(store, bits[0])

    step = chunk_rows(hidden, 128)
    down_local, down_flip, ddown_local, ddown_flip, token = call(
        load_down_kernel(step),
        [
            pltpu.VMEM((hidden, width), bf16),
            pltpu.VMEM((width, hidden), bf16),
            pltpu.VMEM((hidden, width), bf16),
            pltpu.VMEM((width, hidden), bf16),
            ((8, 128), f32),
        ],
        grant,
        down_weight[0],
        down_dir[0],
        specs=[HBM, HBM],
        scratch=[pltpu.SemaphoreType.DMA((2 * (hidden // step),))],
    )
    moved_forward, moved_backward, far, token = lax.optimization_barrier(
        (moved_forward, moved_backward, far, token)
    )
    stores = [store, far]
    for bit in bits[1:]:
        stores = stores + [swapped(b, bit) for b in stores]
    own = call(
        arrive_kernel(rows),
        [((4 * rows, width), bf16)],
        4,
        moved_forward,
        moved_backward,
        edge,
        token,
    )[0]
    own_far = swapped(own, bits[0])
    step = chunk_rows(width, 768)
    m_all, q_all, slope, bend, up_local, dup_local = call(
        stash_kernel(count, rows, step),
        [
            ((width, pairs), bf16),
            ((hidden, pairs), bf16),
            ((TICKS * tokens, hidden), f32),
            ((TICKS * tokens, hidden), f32),
            pltpu.VMEM((width, hidden), bf16),
            pltpu.VMEM((width, hidden), bf16),
        ],
        grant,
        *stores,
        gain,
        up_weight[0],
        up_dir[0],
        specs=[VM] * (count + 1) + [HBM, HBM],
        scratch=[
            pltpu.VMEM((pairs, width), bf16),
            pltpu.VMEM((TICKS * tokens, width), bf16),
            pltpu.VMEM((pairs, hidden), f32),
            pltpu.VMEM((TICKS * tokens, hidden), f32),
            pltpu.SemaphoreType.DMA((2 * (width // step),)),
        ],
    )
    weights = (
        up_local,
        dup_local,
        down_local,
        down_flip,
        ddown_local,
        ddown_flip,
    )
    own_far, slope = lax.optimization_barrier((own_far, slope))
    blocks = [own, own_far]
    for bit in bits[1:]:
        blocks = blocks + [swapped(b, bit) for b in blocks]
    own_now, other_now = blocks[0], blocks[half]
    z_list, adj_list = [], []
    for tick in range(TICKS):
        last = tick + 1 == TICKS
        split = half if last else count
        width_of = 4 if last else 2
        outs = [
            ((split * width_of * rows, width), f32),
            ((split * width_of * rows, width), bf16),
            ((2 * tokens, hidden), bf16),
            ((2 * tokens, width), bf16),
        ]
        if tick:
            outs.append(((4 * rows, width), bf16))
        keep, send, z_pair, adj, *rest = call(
            tick_kernel(count, rows, tick),
            outs,
            grant,
            *blocks,
            gain,
            *weights,
            slope,
            bend,
            scratch=[pltpu.VMEM((2 * tokens, width), bf16), pltpu.VMEM((2 * tokens, hidden), bf16)],
        )
        if tick:
            own_now = rest[0]
        z_list.append(z_pair)
        adj_list.append(adj)
        for bit in bits[::-1][:-1]:
            got = swapped(send, bit)
            part = keep.shape[0] // 2
            keep, send = call(
                add_body, [((part, width), f32), ((part, width), bf16)], 4, keep, got
            )
        got = swapped(send, bits[0])
        if last:
            ended = call(
                last_kernel(rows, tick),
                [((1, rows, width), bf16)] * 4,
                4,
                keep,
                got,
                own_now,
                store,
                gain,
            )
        else:
            unit = call(
                unit_kernel(rows, tick),
                [((4 * rows, width), bf16)],
                4,
                keep,
                got,
                own_now,
                other_now,
                store,
                stores[half],
                gain,
            )[0]
            arrived = parity_moved(unit)
            mine = gather_blocks(arrived, bits[:-1])
            theirs = [swapped(u, bits[-1]) for u in mine]
            blocks = mine + theirs + stores

    steps = next(
        n for n in range(6, 0, -1) if width % (8 * n) == 0 and hidden % (8 * n) == 0
    )
    total_up, total_down = pl.pallas_call(
        curvature_kernel(steps),
        in_specs=[VM] * (2 + 2 * TICKS),
        out_specs=[HBM, HBM],
        out_shape=[
            jax.ShapeDtypeStruct((width, hidden), bf16),
            jax.ShapeDtypeStruct((hidden, width), bf16),
        ],
        scratch_shapes=[
            pltpu.VMEM((width, hidden), bf16),
            pltpu.VMEM((hidden, width), bf16),
            pltpu.SemaphoreType.DMA((2 * steps,)),
        ],
        compiler_params=params(11),
    )(m_all, q_all, *z_list, *adj_list)
    return (*ended, total_up[None], total_down[None])


def solution(mesh):
    in_specs = (
        P("section", "dp", None),
        P("section", "dp", None),
        P("section", "dp", None),
        P("section", "dp", None),
        P(None, "dp", None),
        P(None, "dp", None),
        P("section", None, "dp", None),
        P("section", None, "dp", None),
        P("section", None),
        P("section", None, "dp"),
        P("section", "dp", None),
        P("section", None, "dp"),
        P("section", "dp", None),
    )
    out_specs = (
        P("section", "dp", None),
        P("section", "dp", None),
        P("section", "dp", None),
        P("section", "dp", None),
        P("section", None, "dp"),
        P("section", "dp", None),
    )
    return jax.shard_map(shards, mesh=mesh, in_specs=in_specs, out_specs=out_specs, check_vma=False)
```

```python
import jax
import jax.numpy as jnp
from jax import lax
from jax.experimental import pallas as pl
from jax.experimental.pallas import tpu as pltpu
from jax.sharding import PartitionSpec as P

TICKS = 2


sqrt_two_over_pi = 0.7978845608028654
cubic_coef = 0.044715
norm_eps = 1e-06

bf16 = jnp.bfloat16
f32 = jnp.float32
VM = pl.BlockSpec(memory_space=pltpu.VMEM)
HBM = pl.BlockSpec(memory_space=pltpu.HBM)


def params(mib):
    return pltpu.CompilerParams(vmem_limit_bytes=mib * 2**20)


def passed_along(value, axis, steps):
    count = lax.axis_size(axis)
    leading, last = (max(0, -steps), min(count, count - steps))
    return lax.ppermute(value, axis, [(source, source + steps) for source in range(leading, last)])


def swapped(value, bit):
    count = lax.axis_size("dp")
    return lax.ppermute(value, "dp", [(source, source ^ bit) for source in range(count)])


def dp_bits():
    count = lax.axis_size("dp")
    bits = []
    bit = count // 2
    while bit:
        bits.append(bit)
        bit //= 2
    return bits


def gather_blocks(block, bits):
    blocks = [block]
    for bit in bits:
        blocks = blocks + [swapped(b, bit) for b in blocks]
    return blocks


def parity_moved(value):
    sections, count = (lax.axis_size("section"), lax.axis_size("dp"))
    pairs = []
    for section in range(sections):
        for member in range(count):
            target = section + (1 if member % 2 == 0 else -1)
            if 0 <= target < sections:
                pairs.append((section * count + member, target * count + member))
    return lax.ppermute(value, ("section", "dp"), pairs)


def gelu_parts(linear):
    inner_arg = sqrt_two_over_pi * (linear + cubic_coef * linear * linear * linear)
    first_slope = sqrt_two_over_pi * (1.0 + 3.0 * cubic_coef * linear * linear)
    second_slope = 6.0 * sqrt_two_over_pi * cubic_coef * linear
    tanh_value = jnp.tanh(inner_arg)
    sech_square = 1.0 - tanh_value * tanh_value
    gelu_value = 0.5 * linear * (1.0 + tanh_value)
    gelu_first = 0.5 * (1.0 + tanh_value) + 0.5 * linear * sech_square * first_slope
    gelu_second = sech_square * (
        first_slope - linear * tanh_value * first_slope * first_slope + 0.5 * linear * second_slope
    )
    return (gelu_value, gelu_first, gelu_second)


def matrix_product(left, right):
    return jnp.dot(left, right, preferred_element_type=f32)


def product_last(left, right):
    return lax.dot_general(left, right, (((1,), (1,)), ((), ())), preferred_element_type=f32)


def product_first(left, right):
    return lax.dot_general(left, right, (((0,), (0,)), ((), ())), preferred_element_type=f32)


def norm_stats(values, values_tan):
    inverse = lax.rsqrt(jnp.mean(values * values, axis=-1, keepdims=True) + norm_eps)
    inverse_tan = -(inverse * inverse * inverse) * jnp.mean(
        values * values_tan, axis=-1, keepdims=True
    )
    return (inverse, inverse_tan)


def norm_rows(values, values_tan, gain_wide):
    inverse, inverse_tan = norm_stats(values, values_tan)
    normed = values * inverse * gain_wide
    normed_tan = (values_tan * inverse + values * inverse_tan) * gain_wide
    return (normed, normed_tan)


def piece(block, index, rows):
    return block[index * rows : (index + 1) * rows, :].astype(f32)


def pick(blocks, index, rows):
    return jnp.concatenate([piece(b, index, rows) for b in blocks], axis=0)


def pack_kernel(rows):
    def body(*refs):
        act, act_tan, adj, adj_tan, fresh, loss, stash, stash_tan, gain = refs[:9]
        keep, send, store, gain_out = refs[9:13]
        fwd, bwd, edge, sems = refs[13:]
        pairs = [
            (act.at[0], fwd.at[pl.ds(0, rows)]),
            (act_tan.at[0], fwd.at[pl.ds(rows, rows)]),
            (adj.at[0], bwd.at[pl.ds(0, rows)]),
            (adj_tan.at[0], bwd.at[pl.ds(rows, rows)]),
            (gain, gain_out),
        ]
        for tick in range(TICKS):
            at = 2 * tick * rows
            pairs.append((stash.at[0, tick], store.at[pl.ds(at, rows)]))
            pairs.append((stash_tan.at[0, tick], store.at[pl.ds(at + rows, rows)]))
            pairs.append((fresh.at[tick], edge.at[pl.ds(at, rows)]))
            pairs.append((loss.at[tick], edge.at[pl.ds(at + rows, rows)]))
        copies = [pltpu.make_async_copy(a, b, sems.at[i]) for i, (a, b) in enumerate(pairs)]
        start_all(copies)
        for copy in copies:
            copy.wait()
        even = (lax.axis_index("dp") & 1) == 0
        ahead, behind = (fwd[...].astype(f32), bwd[...].astype(f32))
        keep[...] = jnp.where(even, ahead, behind).astype(bf16)
        send[...] = jnp.where(even, behind, ahead).astype(bf16)
        section = lax.axis_index("section")
        at_first = section == 0
        at_last = section == lax.axis_size("section") - 1
        for k in range(2 * TICKS):
            masked = jnp.where(at_first if k % 2 == 0 else at_last, piece(edge, k, rows), 0.0)
            base = (2 * TICKS + k) * rows
            store[base : base + rows, :] = masked.astype(bf16)

    return body


def join_body(keep_ref, got_ref, unit_ref):
    half = keep_ref.shape[0]
    unit_ref[:half, :] = keep_ref[...]
    unit_ref[half:, :] = got_ref[...]


def pass_body(unit_ref, far_ref, token_ref, out_ref, far_out_ref):
    out_ref[...] = unit_ref[...]
    far_out_ref[...] = far_ref[...]


def start_all(copies):
    for copy in copies:
        copy.start()


def chunk_rows(total, limit):
    sizes = [c for c in range(128, limit + 1, 128) if total % c == 0]
    return sizes[-1] if sizes else total


def load_down_kernel(step):
    def body(down_hbm, ddown_hbm, down_ref, down_t_ref, ddown_ref, ddown_t_ref, token, sems):
        token[...] = jnp.zeros_like(token)
        steps = down_hbm.shape[0] // step
        loads = ((down_hbm, down_ref, down_t_ref), (ddown_hbm, ddown_ref, ddown_t_ref))

        def copies(i):
            span = pl.ds(pl.multiple_of(i * step, step), step)
            return [
                pltpu.make_async_copy(src.at[span], dst.at[span], sems.at[2 * i + k])
                for k, (src, dst, _) in enumerate(loads)
            ]

        lax.fori_loop(0, steps, lambda i, c: start_all(copies(i)), None)

        def work(i, carry):
            span = pl.ds(pl.multiple_of(i * step, step), step)
            for copy, (_, dst, flip) in zip(copies(i), loads):
                copy.wait()
                flip[:, span] = dst[span, :].T

        lax.fori_loop(0, steps, work, None)

    return body


def stash_kernel(count, rows, step):
    tokens = count * rows

    def body(*refs):
        blocks = refs[:count]
        gain_ref, up_hbm, dup_hbm = refs[count : count + 3]
        (
            m_ref,
            q_ref,
            slope_ref,
            bend_ref,
            up_ref,
            dup_ref,
            stack,
            plain,
            both,
            side,
            sems,
        ) = refs[count + 3 :]
        steps = up_hbm.shape[0] // step
        loads = ((up_hbm, up_ref), (dup_hbm, dup_ref))

        def copies(i):
            span = pl.ds(pl.multiple_of(i * step, step), step)
            return [
                pltpu.make_async_copy(src.at[span], dst.at[span], sems.at[2 * i + k])
                for k, (src, dst) in enumerate(loads)
            ]

        lax.fori_loop(0, steps, lambda i, c: start_all(copies(i)), None)
        gain_wide = gain_ref[...].astype(f32)
        for tick in range(TICKS):
            normed, normed_tan = norm_rows(
                pick(blocks, 2 * tick, rows), pick(blocks, 2 * tick + 1, rows), gain_wide
            )
            base = 2 * tick * tokens
            stack[base : base + tokens, :] = normed_tan.astype(bf16)
            stack[base + tokens : base + 2 * tokens, :] = normed.astype(bf16)
            plain[tick * tokens : (tick + 1) * tokens, :] = normed.astype(bf16)
        m_ref[...] = stack[...].T
        both[...] = jnp.zeros_like(both)
        side[...] = jnp.zeros_like(side)

        def work(i, carry):
            span = pl.ds(pl.multiple_of(i * step, step), step)
            sides = zip(copies(i), loads, ((stack, both), (plain, side)))
            for copy, (_, dst), (left, total) in sides:
                copy.wait()
                total[...] += matrix_product(left[:, span], dst[span, :])

        lax.fori_loop(0, steps, work, None)
        for tick in range(TICKS):
            base = 2 * tick * tokens
            linear = both[base + tokens : base + 2 * tokens, :]
            linear_tan = (
                both[base : base + tokens, :] + side[tick * tokens : (tick + 1) * tokens, :]
            )
            value, first, second = gelu_parts(linear)
            q_pair = jnp.concatenate([first * linear_tan, value], axis=0).astype(bf16)
            q_ref[:, base : base + 2 * tokens] = q_pair.T
            slope_ref[tick * tokens : (tick + 1) * tokens, :] = first
            bend_ref[tick * tokens : (tick + 1) * tokens, :] = second * linear_tan

    return body


def tick_kernel(count, rows, tick):
    tokens = count * rows
    half = count // 2
    n_in = 2 * count

    def body(*refs):
        blocks = refs[:n_in]
        (
            gain_ref,
            up_ref,
            dup_ref,
            down_ref,
            down_t_ref,
            ddown_ref,
            ddown_t_ref,
            slope_ref,
            bend_ref,
        ) = refs[n_in : n_in + 9]
        outs = refs[n_in + 9 : -2]
        pair_ref, hid_ref = refs[-2:]
        keep_ref, send_ref, z_ref, adj_ref = outs[:4]
        even = (lax.axis_index("dp") & 1) == 0
        gain_wide = gain_ref[...].astype(f32)
        mine, theirs, edges = (blocks[:half], blocks[half:count], blocks[count:])
        values = []
        for chain in range(2):
            for a in range(2):
                here = [piece(u, 2 * b + a, rows) for b in (0, 1) for u in mine]
                there = [piece(u, 2 * b + a, rows) for b in (1, 0) for u in theirs]
                here = jnp.concatenate(here, axis=0)
                there = jnp.concatenate(there, axis=0)
                first, second = (here, there) if chain == 0 else (there, here)
                value = jnp.where(even, first, second)
                if a == 0:
                    value = value + pick(edges, 2 * TICKS + 2 * tick + chain, rows)
                values.append(value)
        for out, k in zip(outs[4:], (0, half)):
            for a in range(4):
                out[a * rows : (a + 1) * rows, :] = values[a][k * rows : (k + 1) * rows].astype(
                    bf16
                )
        normed, normed_tan = norm_rows(values[0], values[1], gain_wide)
        pair_ref[:tokens, :] = normed.astype(bf16)
        pair_ref[tokens:, :] = normed_tan.astype(bf16)
        adj_ref[:tokens, :] = values[2].astype(bf16)
        adj_ref[tokens:, :] = values[3].astype(bf16)
        hidden, width = up_ref.shape[1], up_ref.shape[0]
        size = hidden
        base = tick * tokens

        def inner(i, carry):
            at = i * size if hidden % size == 0 else jnp.minimum(i * size, hidden - size)
            span = pl.ds(pl.multiple_of(at, 128) if size != hidden else 0, size)
            both = matrix_product(pair_ref[...], up_ref[:, span])
            side = matrix_product(pair_ref[:tokens, :], dup_ref[:, span])
            e_both = matrix_product(adj_ref[...], down_t_ref[:, span])
            e_side = matrix_product(adj_ref[:tokens, :], ddown_t_ref[:, span])
            value, first, _ = gelu_parts(both[:tokens])
            hid_ref[:tokens, span] = value.astype(bf16)
            hid_ref[tokens:, span] = (first * (both[tokens:] + side)).astype(bf16)
            upstream = e_both[:tokens]
            slope = slope_ref[base : base + tokens, span]
            bend = bend_ref[base : base + tokens, span]
            z_ref[:tokens, span] = (upstream * slope).astype(bf16)
            z_ref[tokens:, span] = ((e_both[tokens:] + e_side) * slope + upstream * bend).astype(
                bf16
            )

        lax.fori_loop(0, -(-hidden // size), inner, None)
        size_out = 1152 if width % 1152 == 0 else width
        order = [k for j in range(half) for k in (j, j + half)]

        def outer(i, carry):
            span = pl.ds(pl.multiple_of(i * size_out, size_out), size_out)
            p_both = matrix_product(hid_ref[...], down_ref[:, span])
            p_side = matrix_product(hid_ref[:tokens, :], ddown_ref[:, span])
            t_both = product_last(z_ref[...], up_ref[span, :])
            t_side = product_last(z_ref[:tokens, :], dup_ref[span, :])
            parts = (
                p_both[:tokens],
                p_both[tokens:] + p_side,
                t_both[:tokens],
                t_both[tokens:] + t_side,
            )
            if tick + 1 == TICKS:
                for k in range(count):
                    for a in range(4):
                        part = parts[a][k * rows : (k + 1) * rows]
                        if k < half:
                            at = (4 * k + a) * rows
                            keep_ref[at : at + rows, span] = part
                        else:
                            at = (4 * (k - half) + a) * rows
                            send_ref[at : at + rows, span] = part.astype(bf16)
            else:
                kept = [jnp.where(even, parts[a], parts[a + 2]) for a in range(2)]
                sent = [jnp.where(even, parts[a + 2], parts[a]) for a in range(2)]
                for i, k in enumerate(order):
                    for a in range(2):
                        at = (2 * i + a) * rows
                        keep_ref[at : at + rows, span] = kept[a][k * rows : (k + 1) * rows]
                        at = (2 * (i ^ 1) + a) * rows
                        send_ref[at : at + rows, span] = sent[a][k * rows : (k + 1) * rows].astype(
                            bf16
                        )

        lax.fori_loop(0, width // size_out, outer, None)

    return body


def add_body(keep_ref, got_ref, low_ref, high_ref):
    half = keep_ref.shape[0] // 2
    low_ref[...] = keep_ref[:half, :] + got_ref[:half, :].astype(f32)
    high_ref[...] = (keep_ref[half:, :] + got_ref[half:, :].astype(f32)).astype(bf16)


def norm_back(values, values_tan, gain_wide, arriving, arriving_tan, summed, summed_tan):
    inverse, inverse_tan = norm_stats(values, values_tan)
    weighted = summed * gain_wide
    weighted_tan = summed_tan * gain_wide
    moment = jnp.mean(values * weighted, axis=-1, keepdims=True)
    moment_tan = jnp.mean(values_tan * weighted + values * weighted_tan, axis=-1, keepdims=True)
    inverse_cube = inverse * inverse * inverse
    returned = arriving + inverse * weighted - inverse_cube * values * moment
    returned_tan = (
        arriving_tan
        + inverse_tan * weighted
        + inverse * weighted_tan
        - 3.0 * inverse * inverse * inverse_tan * values * moment
        - inverse_cube * values_tan * moment
        - inverse_cube * values * moment_tan
    )
    return (returned, returned_tan)


def unit_kernel(rows, tick):
    def body(keep_ref, got_ref, own_ref, other_ref, stash_ref, stash_other_ref, gain_ref, out_ref):
        even = (lax.axis_index("dp") & 1) == 0
        total = keep_ref[...] + got_ref[...].astype(f32)
        sources = ((own_ref, stash_ref), (other_ref, stash_other_ref))

        @pl.when(even)
        def _():
            for b, (block, _) in enumerate(sources):
                for a in range(2):
                    at = (2 * b + a) * rows
                    out_ref[at : at + rows, :] = (
                        piece(block, a, rows) + total[at : at + rows]
                    ).astype(bf16)

        @pl.when(jnp.logical_not(even))
        def _():
            gain_wide = gain_ref[...].astype(f32)
            for b, (block, store) in enumerate(sources):
                at = 2 * b * rows
                returned = norm_back(
                    piece(store, 2 * tick, rows),
                    piece(store, 2 * tick + 1, rows),
                    gain_wide,
                    piece(block, 2, rows),
                    piece(block, 3, rows),
                    total[at : at + rows],
                    total[at + rows : at + 2 * rows],
                )
                for a in range(2):
                    out_ref[at + a * rows : at + (a + 1) * rows, :] = returned[a].astype(bf16)

    return body


def last_kernel(rows, tick):
    def body(keep_ref, got_ref, own_ref, stash_ref, gain_ref, *outs):
        total = keep_ref[...] + got_ref[...].astype(f32)
        parts = [total[a * rows : (a + 1) * rows] for a in range(4)]
        for a in range(2):
            outs[a][0] = (piece(own_ref, a, rows) + parts[a]).astype(bf16)
        returned = norm_back(
            piece(stash_ref, 2 * tick, rows),
            piece(stash_ref, 2 * tick + 1, rows),
            gain_ref[...].astype(f32),
            piece(own_ref, 2, rows),
            piece(own_ref, 3, rows),
            parts[2],
            parts[3],
        )
        for a in range(2):
            outs[2 + a][0] = returned[a].astype(bf16)

    return body


def curvature_kernel(steps):
    def body(*refs):
        m_ref, q_ref = refs[:2]
        z_refs, adj_refs = refs[2 : 2 + TICKS], refs[2 + TICKS : 2 + 2 * TICKS]
        up_hbm, down_hbm, up_ref, down_ref, sems = refs[2 + 2 * TICKS :]
        jobs = ((m_ref, z_refs, up_ref, up_hbm), (q_ref, adj_refs, down_ref, down_hbm))

        def copies(i):
            made = []
            for k, (_, _, ref, hbm) in enumerate(jobs):
                size = ref.shape[0] // steps
                span = pl.ds(pl.multiple_of(i * size, size), size)
                made.append(pltpu.make_async_copy(ref.at[span], hbm.at[span], sems.at[2 * i + k]))
            return made

        def work(i, carry):
            for copy, (left, rights, ref, _) in zip(copies(i), jobs):
                size = ref.shape[0] // steps
                span = pl.ds(pl.multiple_of(i * size, size), size)
                right = jnp.concatenate([r[...] for r in rights], axis=0)
                ref[span, :] = matrix_product(left[span, :], right).astype(bf16)
                copy.start()

        lax.fori_loop(0, steps, work, None)

        def finish(i, carry):
            for copy in copies(i):
                copy.wait()

        lax.fori_loop(0, steps, finish, None)

    return body


def call(body, outs, mib, *operands, specs=None, scratch=()):
    operands = [
        pltpu.with_memory_space_constraint(x, pltpu.HBM) if specs and specs[i] is HBM else x
        for i, x in enumerate(operands)
    ]
    return pl.pallas_call(
        body,
        in_specs=specs or [VM] * len(operands),
        out_specs=[VM] * len(outs),
        out_shape=[jax.ShapeDtypeStruct(*o) if isinstance(o, tuple) else o for o in outs],
        scratch_shapes=scratch,
        compiler_params=params(mib),
    )(*operands)


def shards(
    carry_act,
    carry_act_tan,
    carry_adj,
    carry_adj_tan,
    fresh_act,
    loss_cot,
    stash_act,
    stash_act_tan,
    norm_gain,
    up_weight,
    down_weight,
    up_dir,
    down_dir,
):
    count = lax.axis_size("dp")
    half = count // 2
    bits = dp_bits()
    rows, width = carry_act.shape[1:]
    hidden = up_weight.shape[2]
    tokens = count * rows
    pairs = 2 * TICKS * tokens
    grant = max(6, tokens // 5)

    keep, send, store, gain = call(
        pack_kernel(rows),
        [
            ((2 * rows, width), bf16),
            ((2 * rows, width), bf16),
            ((4 * TICKS * rows, width), bf16),
            ((1, width), bf16),
        ],
        grant,
        carry_act,
        carry_act_tan,
        carry_adj,
        carry_adj_tan,
        fresh_act,
        loss_cot,
        stash_act,
        stash_act_tan,
        norm_gain,
        specs=[HBM] * 9,
        scratch=[
            pltpu.VMEM((2 * rows, width), bf16),
            pltpu.VMEM((2 * rows, width), bf16),
            pltpu.VMEM((2 * TICKS * rows, width), bf16),
            pltpu.SemaphoreType.DMA((5 + 4 * TICKS,)),
        ],
    )
    got = swapped(send, bits[-1])
    unit = call(join_body, [((4 * rows, width), bf16)], grant, keep, got)[0]
    arrived = parity_moved(unit)
    far = swapped(store, bits[0])

    step = chunk_rows(hidden, 128)
    down_local, down_flip, ddown_local, ddown_flip, token = call(
        load_down_kernel(step),
        [
            pltpu.VMEM((hidden, width), bf16),
            pltpu.VMEM((width, hidden), bf16),
            pltpu.VMEM((hidden, width), bf16),
            pltpu.VMEM((width, hidden), bf16),
            ((8, 128), f32),
        ],
        grant,
        down_weight[0],
        down_dir[0],
        specs=[HBM, HBM],
        scratch=[pltpu.SemaphoreType.DMA((2 * (hidden // step),))],
    )
    arrived, far = call(
        pass_body, [(arrived.shape, bf16), (far.shape, bf16)], grant, arrived, far, token
    )
    stores = [store, far]
    for bit in bits[1:]:
        stores = stores + [swapped(b, bit) for b in stores]
    mine = gather_blocks(arrived, bits[:-1])
    step = chunk_rows(width, 768)
    m_all, q_all, slope, bend, up_local, dup_local = call(
        stash_kernel(count, rows, step),
        [
            ((width, pairs), bf16),
            ((hidden, pairs), bf16),
            ((TICKS * tokens, hidden), f32),
            ((TICKS * tokens, hidden), f32),
            pltpu.VMEM((width, hidden), bf16),
            pltpu.VMEM((width, hidden), bf16),
        ],
        grant,
        *stores,
        gain,
        up_weight[0],
        up_dir[0],
        specs=[VM] * (count + 1) + [HBM, HBM],
        scratch=[
            pltpu.VMEM((pairs, width), bf16),
            pltpu.VMEM((TICKS * tokens, width), bf16),
            pltpu.VMEM((pairs, hidden), f32),
            pltpu.VMEM((TICKS * tokens, hidden), f32),
            pltpu.SemaphoreType.DMA((2 * (width // step),)),
        ],
    )
    weights = (
        up_local,
        dup_local,
        down_local,
        down_flip,
        ddown_local,
        ddown_flip,
    )
    last_mine, slope = lax.optimization_barrier((mine[-1], slope))
    mine = mine[:-1] + [last_mine]
    theirs = [swapped(u, bits[-1]) for u in mine]
    blocks = mine + theirs + stores
    z_list, adj_list = [], []
    for tick in range(TICKS):
        last = tick + 1 == TICKS
        split = half if last else count
        width_of = 4 if last else 2
        outs = [
            ((split * width_of * rows, width), f32),
            ((split * width_of * rows, width), bf16),
            ((2 * tokens, hidden), bf16),
            ((2 * tokens, width), bf16),
        ]
        outs = outs + [((4 * rows, width), bf16)] * (1 if last else 2)
        keep, send, z_pair, adj, *rest = call(
            tick_kernel(count, rows, tick),
            outs,
            grant,
            *blocks,
            gain,
            *weights,
            slope,
            bend,
            scratch=[pltpu.VMEM((2 * tokens, width), bf16), pltpu.VMEM((2 * tokens, hidden), bf16)],
        )
        own_now = rest[0]
        z_list.append(z_pair)
        adj_list.append(adj)
        for bit in bits[::-1][:-1]:
            got = swapped(send, bit)
            part = keep.shape[0] // 2
            keep, send = call(
                add_body, [((part, width), f32), ((part, width), bf16)], 4, keep, got
            )
        got = swapped(send, bits[0])
        if last:
            ended = call(
                last_kernel(rows, tick),
                [((1, rows, width), bf16)] * 4,
                4,
                keep,
                got,
                own_now,
                store,
                gain,
            )
        else:
            unit = call(
                unit_kernel(rows, tick),
                [((4 * rows, width), bf16)],
                4,
                keep,
                got,
                own_now,
                rest[1],
                store,
                stores[half],
                gain,
            )[0]
            arrived = parity_moved(unit)
            mine = gather_blocks(arrived, bits[:-1])
            theirs = [swapped(u, bits[-1]) for u in mine]
            blocks = mine + theirs + stores

    steps = next(
        n for n in range(6, 0, -1) if width % (8 * n) == 0 and hidden % (8 * n) == 0
    )
    total_up, total_down = pl.pallas_call(
        curvature_kernel(steps),
        in_specs=[VM] * (2 + 2 * TICKS),
        out_specs=[HBM, HBM],
        out_shape=[
            jax.ShapeDtypeStruct((width, hidden), bf16),
            jax.ShapeDtypeStruct((hidden, width), bf16),
        ],
        scratch_shapes=[
            pltpu.VMEM((width, hidden), bf16),
            pltpu.VMEM((hidden, width), bf16),
            pltpu.SemaphoreType.DMA((2 * steps,)),
        ],
        compiler_params=params(11),
    )(m_all, q_all, *z_list, *adj_list)
    return (*ended, total_up[None], total_down[None])


def solution(mesh):
    in_specs = (
        P("section", "dp", None),
        P("section", "dp", None),
        P("section", "dp", None),
        P("section", "dp", None),
        P(None, "dp", None),
        P(None, "dp", None),
        P("section", None, "dp", None),
        P("section", None, "dp", None),
        P("section", None),
        P("section", None, "dp"),
        P("section", "dp", None),
        P("section", None, "dp"),
        P("section", "dp", None),
    )
    out_specs = (
        P("section", "dp", None),
        P("section", "dp", None),
        P("section", "dp", None),
        P("section", "dp", None),
        P("section", None, "dp"),
        P("section", "dp", None),
    )
    return jax.shard_map(shards, mesh=mesh, in_specs=in_specs, out_specs=out_specs, check_vma=False)
```

```python
import jax
import jax.numpy as jnp
from jax import lax
from jax.experimental import pallas as pl
from jax.experimental.pallas import tpu as pltpu
from jax.sharding import PartitionSpec as P

TICKS = 2


sqrt_two_over_pi = 0.7978845608028654
cubic_coef = 0.044715
norm_eps = 1e-06

bf16 = jnp.bfloat16
f32 = jnp.float32
VM = pl.BlockSpec(memory_space=pltpu.VMEM)
HBM = pl.BlockSpec(memory_space=pltpu.HBM)


def params(mib):
    return pltpu.CompilerParams(vmem_limit_bytes=mib * 2**20)


def passed_along(value, axis, steps):
    count = lax.axis_size(axis)
    leading, last = (max(0, -steps), min(count, count - steps))
    return lax.ppermute(value, axis, [(source, source + steps) for source in range(leading, last)])


def swapped(value, bit):
    count = lax.axis_size("dp")
    return lax.ppermute(value, "dp", [(source, source ^ bit) for source in range(count)])


def dp_bits():
    count = lax.axis_size("dp")
    bits = []
    bit = count // 2
    while bit:
        bits.append(bit)
        bit //= 2
    return bits


def gather_blocks(block, bits):
    blocks = [block]
    for bit in bits:
        blocks = blocks + [swapped(b, bit) for b in blocks]
    return blocks


def parity_moved(value):
    sections, count = (lax.axis_size("section"), lax.axis_size("dp"))
    pairs = []
    for section in range(sections):
        for member in range(count):
            target = section + (1 if member % 2 == 0 else -1)
            if 0 <= target < sections:
                pairs.append((section * count + member, target * count + member))
    return lax.ppermute(value, ("section", "dp"), pairs)


def gelu_parts(linear):
    inner_arg = sqrt_two_over_pi * (linear + cubic_coef * linear * linear * linear)
    first_slope = sqrt_two_over_pi * (1.0 + 3.0 * cubic_coef * linear * linear)
    second_slope = 6.0 * sqrt_two_over_pi * cubic_coef * linear
    tanh_value = jnp.tanh(inner_arg)
    sech_square = 1.0 - tanh_value * tanh_value
    gelu_value = 0.5 * linear * (1.0 + tanh_value)
    gelu_first = 0.5 * (1.0 + tanh_value) + 0.5 * linear * sech_square * first_slope
    gelu_second = sech_square * (
        first_slope - linear * tanh_value * first_slope * first_slope + 0.5 * linear * second_slope
    )
    return (gelu_value, gelu_first, gelu_second)


def matrix_product(left, right):
    return jnp.dot(left, right, preferred_element_type=f32)


def product_last(left, right):
    return lax.dot_general(left, right, (((1,), (1,)), ((), ())), preferred_element_type=f32)


def product_first(left, right):
    return lax.dot_general(left, right, (((0,), (0,)), ((), ())), preferred_element_type=f32)


def norm_stats(values, values_tan):
    inverse = lax.rsqrt(jnp.mean(values * values, axis=-1, keepdims=True) + norm_eps)
    inverse_tan = -(inverse * inverse * inverse) * jnp.mean(
        values * values_tan, axis=-1, keepdims=True
    )
    return (inverse, inverse_tan)


def norm_rows(values, values_tan, gain_wide):
    inverse, inverse_tan = norm_stats(values, values_tan)
    normed = values * inverse * gain_wide
    normed_tan = (values_tan * inverse + values * inverse_tan) * gain_wide
    return (normed, normed_tan)


def piece(block, index, rows):
    return block[index * rows : (index + 1) * rows, :].astype(f32)


def pick(blocks, index, rows):
    return jnp.concatenate([piece(b, index, rows) for b in blocks], axis=0)


def pack_kernel(rows):
    def body(*refs):
        act, act_tan, adj, adj_tan, fresh, loss, stash, stash_tan, gain = refs[:9]
        keep, send, store, gain_out = refs[9:13]
        fwd, bwd, edge, sems = refs[13:]
        pairs = [
            (act.at[0], fwd.at[pl.ds(0, rows)]),
            (act_tan.at[0], fwd.at[pl.ds(rows, rows)]),
            (adj.at[0], bwd.at[pl.ds(0, rows)]),
            (adj_tan.at[0], bwd.at[pl.ds(rows, rows)]),
            (gain, gain_out),
        ]
        for tick in range(TICKS):
            at = 2 * tick * rows
            pairs.append((stash.at[0, tick], store.at[pl.ds(at, rows)]))
            pairs.append((stash_tan.at[0, tick], store.at[pl.ds(at + rows, rows)]))
            pairs.append((fresh.at[tick], edge.at[pl.ds(at, rows)]))
            pairs.append((loss.at[tick], edge.at[pl.ds(at + rows, rows)]))
        copies = [pltpu.make_async_copy(a, b, sems.at[i]) for i, (a, b) in enumerate(pairs)]
        start_all(copies)
        for copy in copies:
            copy.wait()
        even = (lax.axis_index("dp") & 1) == 0
        ahead, behind = (fwd[...].astype(f32), bwd[...].astype(f32))
        keep[...] = jnp.where(even, ahead, behind).astype(bf16)
        send[...] = jnp.where(even, behind, ahead).astype(bf16)
        section = lax.axis_index("section")
        at_first = section == 0
        at_last = section == lax.axis_size("section") - 1
        for k in range(2 * TICKS):
            masked = jnp.where(at_first if k % 2 == 0 else at_last, piece(edge, k, rows), 0.0)
            base = (2 * TICKS + k) * rows
            store[base : base + rows, :] = masked.astype(bf16)

    return body


def join_body(keep_ref, got_ref, unit_ref):
    half = keep_ref.shape[0]
    unit_ref[:half, :] = keep_ref[...]
    unit_ref[half:, :] = got_ref[...]


def pass_body(unit_ref, far_ref, token_ref, out_ref, far_out_ref):
    out_ref[...] = unit_ref[...]
    far_out_ref[...] = far_ref[...]


def wait_body(unit_ref, token_ref, out_ref):
    out_ref[...] = unit_ref[...]


def start_all(copies):
    for copy in copies:
        copy.start()


def chunk_rows(total, limit):
    sizes = [c for c in range(128, limit + 1, 128) if total % c == 0]
    return sizes[-1] if sizes else total


def load_down_kernel(step):
    def body(down_hbm, ddown_hbm, down_ref, down_t_ref, ddown_ref, ddown_t_ref, token, sems):
        token[...] = jnp.zeros_like(token)
        steps = down_hbm.shape[0] // step
        loads = ((down_hbm, down_ref, down_t_ref), (ddown_hbm, ddown_ref, ddown_t_ref))

        def copies(i):
            span = pl.ds(pl.multiple_of(i * step, step), step)
            return [
                pltpu.make_async_copy(src.at[span], dst.at[span], sems.at[2 * i + k])
                for k, (src, dst, _) in enumerate(loads)
            ]

        lax.fori_loop(0, steps, lambda i, c: start_all(copies(i)), None)

        def work(i, carry):
            span = pl.ds(pl.multiple_of(i * step, step), step)
            for copy, (_, dst, flip) in zip(copies(i), loads):
                copy.wait()
                flip[:, span] = dst[span, :].T

        lax.fori_loop(0, steps, work, None)

    return body


def stash_rows(blocks, gain_ref, tick, rows, stack, plain):
    gain_wide = gain_ref[...].astype(f32)
    normed, normed_tan = norm_rows(
        pick(blocks, 2 * tick, rows), pick(blocks, 2 * tick + 1, rows), gain_wide
    )
    tokens = normed.shape[0]
    stack[:tokens, :] = normed_tan.astype(bf16)
    stack[tokens:, :] = normed.astype(bf16)
    plain[...] = normed.astype(bf16)


def stash_hidden(both, side, slope_ref, bend_ref):
    tokens = side.shape[0]
    linear_tan = both[:tokens] + side
    value, first, second = gelu_parts(both[tokens:])
    slope_ref[...] = first
    bend_ref[...] = second * linear_tan
    return jnp.concatenate([first * linear_tan, value], axis=0).astype(bf16)


def stash_kernel(count, rows, step):
    def body(*refs):
        blocks = refs[:count]
        gain_ref, up_hbm, dup_hbm = refs[count : count + 3]
        m_ref, q_ref, slope_ref, bend_ref, up_ref, dup_ref, plain, both, side, sems = refs[
            count + 3 :
        ]
        steps = up_hbm.shape[0] // step
        loads = ((up_hbm, up_ref), (dup_hbm, dup_ref))

        def copies(i):
            span = pl.ds(pl.multiple_of(i * step, step), step)
            return [
                pltpu.make_async_copy(src.at[span], dst.at[span], sems.at[2 * i + k])
                for k, (src, dst) in enumerate(loads)
            ]

        lax.fori_loop(0, steps, lambda i, c: start_all(copies(i)), None)
        stash_rows(blocks, gain_ref, 0, rows, m_ref, plain)
        both[...] = jnp.zeros_like(both)
        side[...] = jnp.zeros_like(side)

        def work(i, carry):
            span = pl.ds(pl.multiple_of(i * step, step), step)
            sides = zip(copies(i), loads, ((m_ref, both), (plain, side)))
            for copy, (_, dst), (left, total) in sides:
                copy.wait()
                total[...] += matrix_product(left[:, span], dst[span, :])

        lax.fori_loop(0, steps, work, None)
        q_ref[...] = stash_hidden(both[...], side[...], slope_ref, bend_ref)

    return body


def later_kernel(count, rows):
    later = TICKS - 1

    def body(*refs):
        blocks = refs[:count]
        gain_ref, up_ref, dup_ref, m_ref, q_ref, _ = refs[count : count + 6]
        m_out, q_out = refs[count + 6 : count + 8]
        slopes = refs[count + 8 : count + 8 + later]
        bends = refs[count + 8 + later : count + 8 + 2 * later]
        stack, plain = refs[count + 8 + 2 * later :]
        size = m_ref.shape[0]
        m_out[:, :size] = m_ref[...].T
        q_out[:, :size] = q_ref[...].T
        for tick in range(1, TICKS):
            stash_rows(blocks, gain_ref, tick, rows, stack, plain)
            both = matrix_product(stack[...], up_ref[...])
            side = matrix_product(plain[...], dup_ref[...])
            q_pair = stash_hidden(both, side, slopes[tick - 1], bends[tick - 1])
            m_out[:, tick * size : (tick + 1) * size] = stack[...].T
            q_out[:, tick * size : (tick + 1) * size] = q_pair.T

    return body


def tick_kernel(count, rows, tick):
    tokens = count * rows
    half = count // 2
    n_in = 2 * count

    def body(*refs):
        blocks = refs[:n_in]
        (
            gain_ref,
            up_ref,
            dup_ref,
            down_ref,
            down_t_ref,
            ddown_ref,
            ddown_t_ref,
            slope_ref,
            bend_ref,
        ) = refs[n_in : n_in + 9]
        outs = refs[n_in + 9 : -2]
        pair_ref, hid_ref = refs[-2:]
        keep_ref, send_ref, z_ref, adj_ref = outs[:4]
        even = (lax.axis_index("dp") & 1) == 0
        gain_wide = gain_ref[...].astype(f32)
        mine, theirs, edges = (blocks[:half], blocks[half:count], blocks[count:])
        values = []
        for chain in range(2):
            for a in range(2):
                here = [piece(u, 2 * b + a, rows) for b in (0, 1) for u in mine]
                there = [piece(u, 2 * b + a, rows) for b in (1, 0) for u in theirs]
                here = jnp.concatenate(here, axis=0)
                there = jnp.concatenate(there, axis=0)
                first, second = (here, there) if chain == 0 else (there, here)
                value = jnp.where(even, first, second)
                if a == 0:
                    value = value + pick(edges, 2 * TICKS + 2 * tick + chain, rows)
                values.append(value)
        for out, k in zip(outs[4:], (0, half)):
            for a in range(4):
                out[a * rows : (a + 1) * rows, :] = values[a][k * rows : (k + 1) * rows].astype(
                    bf16
                )
        normed, normed_tan = norm_rows(values[0], values[1], gain_wide)
        pair_ref[:tokens, :] = normed.astype(bf16)
        pair_ref[tokens:, :] = normed_tan.astype(bf16)
        adj_ref[:tokens, :] = values[2].astype(bf16)
        adj_ref[tokens:, :] = values[3].astype(bf16)
        hidden, width = up_ref.shape[1], up_ref.shape[0]
        size = hidden
        base = 0

        def inner(i, carry):
            at = i * size if hidden % size == 0 else jnp.minimum(i * size, hidden - size)
            span = pl.ds(pl.multiple_of(at, 128) if size != hidden else 0, size)
            both = matrix_product(pair_ref[...], up_ref[:, span])
            side = matrix_product(pair_ref[:tokens, :], dup_ref[:, span])
            e_both = matrix_product(adj_ref[...], down_t_ref[:, span])
            e_side = matrix_product(adj_ref[:tokens, :], ddown_t_ref[:, span])
            value, first, _ = gelu_parts(both[:tokens])
            hid_ref[:tokens, span] = value.astype(bf16)
            hid_ref[tokens:, span] = (first * (both[tokens:] + side)).astype(bf16)
            upstream = e_both[:tokens]
            slope = slope_ref[base : base + tokens, span]
            bend = bend_ref[base : base + tokens, span]
            z_ref[:tokens, span] = (upstream * slope).astype(bf16)
            z_ref[tokens:, span] = ((e_both[tokens:] + e_side) * slope + upstream * bend).astype(
                bf16
            )

        lax.fori_loop(0, -(-hidden // size), inner, None)
        size_out = 1152 if width % 1152 == 0 else width
        order = [k for j in range(half) for k in (j, j + half)]

        def outer(i, carry):
            span = pl.ds(pl.multiple_of(i * size_out, size_out), size_out)
            p_both = matrix_product(hid_ref[...], down_ref[:, span])
            p_side = matrix_product(hid_ref[:tokens, :], ddown_ref[:, span])
            t_both = product_last(z_ref[...], up_ref[span, :])
            t_side = product_last(z_ref[:tokens, :], dup_ref[span, :])
            parts = (
                p_both[:tokens],
                p_both[tokens:] + p_side,
                t_both[:tokens],
                t_both[tokens:] + t_side,
            )
            if tick + 1 == TICKS:
                for k in range(count):
                    for a in range(4):
                        part = parts[a][k * rows : (k + 1) * rows]
                        if k < half:
                            at = (4 * k + a) * rows
                            keep_ref[at : at + rows, span] = part
                        else:
                            at = (4 * (k - half) + a) * rows
                            send_ref[at : at + rows, span] = part.astype(bf16)
            else:
                kept = [jnp.where(even, parts[a], parts[a + 2]) for a in range(2)]
                sent = [jnp.where(even, parts[a + 2], parts[a]) for a in range(2)]
                for i, k in enumerate(order):
                    for a in range(2):
                        at = (2 * i + a) * rows
                        keep_ref[at : at + rows, span] = kept[a][k * rows : (k + 1) * rows]
                        at = (2 * (i ^ 1) + a) * rows
                        send_ref[at : at + rows, span] = sent[a][k * rows : (k + 1) * rows].astype(
                            bf16
                        )

        lax.fori_loop(0, width // size_out, outer, None)

    return body


def add_body(keep_ref, got_ref, low_ref, high_ref):
    half = keep_ref.shape[0] // 2
    low_ref[...] = keep_ref[:half, :] + got_ref[:half, :].astype(f32)
    high_ref[...] = (keep_ref[half:, :] + got_ref[half:, :].astype(f32)).astype(bf16)


def norm_back(values, values_tan, gain_wide, arriving, arriving_tan, summed, summed_tan):
    inverse, inverse_tan = norm_stats(values, values_tan)
    weighted = summed * gain_wide
    weighted_tan = summed_tan * gain_wide
    moment = jnp.mean(values * weighted, axis=-1, keepdims=True)
    moment_tan = jnp.mean(values_tan * weighted + values * weighted_tan, axis=-1, keepdims=True)
    inverse_cube = inverse * inverse * inverse
    returned = arriving + inverse * weighted - inverse_cube * values * moment
    returned_tan = (
        arriving_tan
        + inverse_tan * weighted
        + inverse * weighted_tan
        - 3.0 * inverse * inverse * inverse_tan * values * moment
        - inverse_cube * values_tan * moment
        - inverse_cube * values * moment_tan
    )
    return (returned, returned_tan)


def unit_kernel(rows, tick):
    def body(keep_ref, got_ref, own_ref, other_ref, stash_ref, stash_other_ref, gain_ref, out_ref):
        even = (lax.axis_index("dp") & 1) == 0
        total = keep_ref[...] + got_ref[...].astype(f32)
        sources = ((own_ref, stash_ref), (other_ref, stash_other_ref))

        @pl.when(even)
        def _():
            for b, (block, _) in enumerate(sources):
                for a in range(2):
                    at = (2 * b + a) * rows
                    out_ref[at : at + rows, :] = (
                        piece(block, a, rows) + total[at : at + rows]
                    ).astype(bf16)

        @pl.when(jnp.logical_not(even))
        def _():
            gain_wide = gain_ref[...].astype(f32)
            for b, (block, store) in enumerate(sources):
                at = 2 * b * rows
                returned = norm_back(
                    piece(store, 2 * tick, rows),
                    piece(store, 2 * tick + 1, rows),
                    gain_wide,
                    piece(block, 2, rows),
                    piece(block, 3, rows),
                    total[at : at + rows],
                    total[at + rows : at + 2 * rows],
                )
                for a in range(2):
                    out_ref[at + a * rows : at + (a + 1) * rows, :] = returned[a].astype(bf16)

    return body


def last_kernel(rows, tick):
    def body(keep_ref, got_ref, own_ref, stash_ref, gain_ref, *outs):
        total = keep_ref[...] + got_ref[...].astype(f32)
        parts = [total[a * rows : (a + 1) * rows] for a in range(4)]
        for a in range(2):
            outs[a][0] = (piece(own_ref, a, rows) + parts[a]).astype(bf16)
        returned = norm_back(
            piece(stash_ref, 2 * tick, rows),
            piece(stash_ref, 2 * tick + 1, rows),
            gain_ref[...].astype(f32),
            piece(own_ref, 2, rows),
            piece(own_ref, 3, rows),
            parts[2],
            parts[3],
        )
        for a in range(2):
            outs[2 + a][0] = returned[a].astype(bf16)

    return body


def curvature_kernel(steps):
    def body(*refs):
        m_ref, q_ref = refs[:2]
        z_refs, adj_refs = refs[2 : 2 + TICKS], refs[2 + TICKS : 2 + 2 * TICKS]
        up_hbm, down_hbm, up_ref, down_ref, sems = refs[2 + 2 * TICKS :]
        jobs = ((m_ref, z_refs, up_ref, up_hbm), (q_ref, adj_refs, down_ref, down_hbm))

        def copies(i):
            made = []
            for k, (_, _, ref, hbm) in enumerate(jobs):
                size = ref.shape[0] // steps
                span = pl.ds(pl.multiple_of(i * size, size), size)
                made.append(pltpu.make_async_copy(ref.at[span], hbm.at[span], sems.at[2 * i + k]))
            return made

        def work(i, carry):
            for copy, (left, rights, ref, _) in zip(copies(i), jobs):
                size = ref.shape[0] // steps
                span = pl.ds(pl.multiple_of(i * size, size), size)
                right = jnp.concatenate([r[...] for r in rights], axis=0)
                ref[span, :] = matrix_product(left[span, :], right).astype(bf16)
                copy.start()

        lax.fori_loop(0, steps, work, None)

        def finish(i, carry):
            for copy in copies(i):
                copy.wait()

        lax.fori_loop(0, steps, finish, None)

    return body


def call(body, outs, mib, *operands, specs=None, scratch=()):
    operands = [
        pltpu.with_memory_space_constraint(x, pltpu.HBM) if specs and specs[i] is HBM else x
        for i, x in enumerate(operands)
    ]
    return pl.pallas_call(
        body,
        in_specs=specs or [VM] * len(operands),
        out_specs=[VM] * len(outs),
        out_shape=[jax.ShapeDtypeStruct(*o) if isinstance(o, tuple) else o for o in outs],
        scratch_shapes=scratch,
        compiler_params=params(mib),
    )(*operands)


def shards(
    carry_act,
    carry_act_tan,
    carry_adj,
    carry_adj_tan,
    fresh_act,
    loss_cot,
    stash_act,
    stash_act_tan,
    norm_gain,
    up_weight,
    down_weight,
    up_dir,
    down_dir,
):
    count = lax.axis_size("dp")
    half = count // 2
    bits = dp_bits()
    rows, width = carry_act.shape[1:]
    hidden = up_weight.shape[2]
    tokens = count * rows
    pairs = 2 * TICKS * tokens
    grant = max(6, tokens // 5)

    keep, send, store, gain = call(
        pack_kernel(rows),
        [
            ((2 * rows, width), bf16),
            ((2 * rows, width), bf16),
            ((4 * TICKS * rows, width), bf16),
            ((1, width), bf16),
        ],
        grant,
        carry_act,
        carry_act_tan,
        carry_adj,
        carry_adj_tan,
        fresh_act,
        loss_cot,
        stash_act,
        stash_act_tan,
        norm_gain,
        specs=[HBM] * 9,
        scratch=[
            pltpu.VMEM((2 * rows, width), bf16),
            pltpu.VMEM((2 * rows, width), bf16),
            pltpu.VMEM((2 * TICKS * rows, width), bf16),
            pltpu.SemaphoreType.DMA((5 + 4 * TICKS,)),
        ],
    )
    got = swapped(send, bits[-1])
    unit = call(join_body, [((4 * rows, width), bf16)], grant, keep, got)[0]
    arrived = parity_moved(unit)
    far = swapped(store, bits[0])

    step = chunk_rows(hidden, 384)
    down_local, down_flip, ddown_local, ddown_flip, token = call(
        load_down_kernel(step),
        [
            pltpu.VMEM((hidden, width), bf16),
            pltpu.VMEM((width, hidden), bf16),
            pltpu.VMEM((hidden, width), bf16),
            pltpu.VMEM((width, hidden), bf16),
            ((8, 128), f32),
        ],
        grant,
        down_weight[0],
        down_dir[0],
        specs=[HBM, HBM],
        scratch=[pltpu.SemaphoreType.DMA((2 * (hidden // step),))],
    )
    arrived, far = call(
        pass_body, [(arrived.shape, bf16), (far.shape, bf16)], grant, arrived, far, token
    )
    stores = [store, far]
    for bit in bits[1:]:
        stores = stores + [swapped(b, bit) for b in stores]
    mine = gather_blocks(arrived, bits[:-1])
    step = chunk_rows(width, 768)
    first_m, first_q, slope, bend, up_local, dup_local = call(
        stash_kernel(count, rows, step),
        [
            ((2 * tokens, width), bf16),
            ((2 * tokens, hidden), bf16),
            ((tokens, hidden), f32),
            ((tokens, hidden), f32),
            pltpu.VMEM((width, hidden), bf16),
            pltpu.VMEM((width, hidden), bf16),
        ],
        grant,
        *stores,
        gain,
        up_weight[0],
        up_dir[0],
        specs=[VM] * (count + 1) + [HBM, HBM],
        scratch=[
            pltpu.VMEM((tokens, width), bf16),
            pltpu.VMEM((2 * tokens, hidden), f32),
            pltpu.VMEM((tokens, hidden), f32),
            pltpu.SemaphoreType.DMA((2 * (width // step),)),
        ],
    )
    weights = (
        up_local,
        dup_local,
        down_local,
        down_flip,
        ddown_local,
        ddown_flip,
    )
    last_mine, slope = lax.optimization_barrier((mine[-1], slope))
    mine = mine[:-1] + [last_mine]
    theirs = [swapped(u, bits[-1]) for u in mine]
    blocks = mine + theirs + stores
    z_list, adj_list = [], []
    for tick in range(TICKS):
        last = tick + 1 == TICKS
        split = half if last else count
        width_of = 4 if last else 2
        outs = [
            ((split * width_of * rows, width), f32),
            ((split * width_of * rows, width), bf16),
            ((2 * tokens, hidden), bf16),
            ((2 * tokens, width), bf16),
        ]
        outs = outs + [((4 * rows, width), bf16)] * (1 if last else 2)
        keep, send, z_pair, adj, *rest = call(
            tick_kernel(count, rows, tick),
            outs,
            grant,
            *blocks,
            gain,
            *weights,
            slope,
            bend,
            scratch=[pltpu.VMEM((2 * tokens, width), bf16), pltpu.VMEM((2 * tokens, hidden), bf16)],
        )
        own_now = rest[0]
        z_list.append(z_pair)
        adj_list.append(adj)
        for bit in bits[::-1][:-1]:
            got = swapped(send, bit)
            part = keep.shape[0] // 2
            keep, send = call(
                add_body, [((part, width), f32), ((part, width), bf16)], 4, keep, got
            )
        got = swapped(send, bits[0])
        if last:
            ended = call(
                last_kernel(rows, tick),
                [((1, rows, width), bf16)] * 4,
                4,
                keep,
                got,
                own_now,
                store,
                gain,
            )
        else:
            unit = call(
                unit_kernel(rows, tick),
                [((4 * rows, width), bf16)],
                4,
                keep,
                got,
                own_now,
                rest[1],
                store,
                stores[half],
                gain,
            )[0]
            arrived = parity_moved(unit)
            if tick == 0:
                m_all, q_all, *curves = call(
                    later_kernel(count, rows),
                    [((width, pairs), bf16), ((hidden, pairs), bf16)]
                    + [((tokens, hidden), f32)] * (2 * (TICKS - 1)),
                    grant,
                    *stores,
                    gain,
                    up_local,
                    dup_local,
                    first_m,
                    first_q,
                    unit,
                    scratch=[
                        pltpu.VMEM((2 * tokens, width), bf16),
                        pltpu.VMEM((tokens, width), bf16),
                    ],
                )
                arrived = call(
                    wait_body, [((4 * rows, width), bf16)], grant, arrived, curves[0]
                )[0]
            slope, bend = curves[tick], curves[tick + TICKS - 1]
            mine = gather_blocks(arrived, bits[:-1])
            theirs = [swapped(u, bits[-1]) for u in mine]
            blocks = mine + theirs + stores

    steps = next(
        n for n in range(6, 0, -1) if width % (8 * n) == 0 and hidden % (8 * n) == 0
    )
    total_up, total_down = pl.pallas_call(
        curvature_kernel(steps),
        in_specs=[VM] * (2 + 2 * TICKS),
        out_specs=[HBM, HBM],
        out_shape=[
            jax.ShapeDtypeStruct((width, hidden), bf16),
            jax.ShapeDtypeStruct((hidden, width), bf16),
        ],
        scratch_shapes=[
            pltpu.VMEM((width, hidden), bf16),
            pltpu.VMEM((hidden, width), bf16),
            pltpu.SemaphoreType.DMA((2 * steps,)),
        ],
        compiler_params=params(11),
    )(m_all, q_all, *z_list, *adj_list)
    return (*ended, total_up[None], total_down[None])


def solution(mesh):
    in_specs = (
        P("section", "dp", None),
        P("section", "dp", None),
        P("section", "dp", None),
        P("section", "dp", None),
        P(None, "dp", None),
        P(None, "dp", None),
        P("section", None, "dp", None),
        P("section", None, "dp", None),
        P("section", None),
        P("section", None, "dp"),
        P("section", "dp", None),
        P("section", None, "dp"),
        P("section", "dp", None),
    )
    out_specs = (
        P("section", "dp", None),
        P("section", "dp", None),
        P("section", "dp", None),
        P("section", "dp", None),
        P("section", None, "dp"),
        P("section", "dp", None),
    )
    return jax.shard_map(shards, mesh=mesh, in_specs=in_specs, out_specs=out_specs, check_vma=False)
```
